256 devices in a mesh: row: 16 (over z_lo, x, core), col: 16 (over y, z_hi).
Axes of the slice: x: 4, y: 4, z: 8 (z_hi: 4, z_lo: 2; z = z_hi * 2 + z_lo), core: 2. Of those that a mesh axis runs over, the one named last changes fastest.
Arguments:
- object_slices: float32 [4, 2, 4096, 4096], P(None, None, 'row', 'col'), may hold values from -2.5 to 2.5
- probe_wave: float32 [2, 128, 128], replicated, may hold values from -4 to 4
- offsets: int32 [16, 16, 4, 2], P('row', 'col'), may hold values from 0 to 255
- active_flags: int32 [16, 16, 4], P('row', 'col'), may hold values 0 or 1
- intensity: float32 [16, 16, 4, 128, 128], P('row', 'col'), may hold values from 0.1 to 3
Outputs:
- updated_object: float32 [4, 2, 4096, 4096], P(None, None, 'row', 'col')
- updated_probe: float32 [2, 128, 128], replicated
The draws below stay inside these ranges and needn't reach their ends.
Inputs may be any that keep to these rules, and one draw needn't show every extreme that they name: `offsets`: each position's centre lies in its own device's tile; its window may reach into neighbouring tiles, diagonal ones included. `active_flags`: positions with flag 0 contribute nothing.
All inputs are finite; a program needn't handle non-finite values. No bound on the sum of `active_flags` on one device may be relied on, other than what follows from the above.
Results may differ from the reference program's by a relative error of at most 0.00018.
Values sent between devices are 32-bit elements; how exact they have to be, the bound alone decides.
A program may use at most 64 MiB of HBM per device.

```python
import math
import jax
import jax.numpy as jnp
from jax import lax

SLICES = 4
PROBE = 128
TILE = 256
POS = 4
ROWS = 4096
COLS = 4096
N_ROW = 16
N_COL = 16


def with_ends(array, stream_key, low, largest):
    longest = array.shape.index(max(array.shape))
    spots = []
    for shift in (0, 1):
        where = [jax.random.randint(jax.random.fold_in(stream_key, axis), (), 0, length) for axis, length in enumerate(array.shape)]
        where[longest] = (where[longest] + shift) % array.shape[longest]
        spots.append(tuple(where))
    return array.at[spots[0]].set(low).at[spots[1]].set(largest)


def shard_levels(stream_key, shape, shards, low, largest):
    def one(position, parts):
        steps = jax.random.uniform(jax.random.fold_in(jax.random.fold_in(stream_key, 6), position), (parts,), jnp.float32, low / len(shards), largest / len(shards))
        return jnp.repeat(jnp.exp(steps), shape[position] // parts).reshape((-1,) + (1,) * (len(shape) - position - 1))

    level = one(*shards[0])
    for cut in shards[1:]:
        level = level * one(*cut)
    return level


def centred(rng, shape, deviation, reach, cuts=(), kind=jnp.bfloat16):
    drawn = jax.random.normal(rng, shape, jnp.float32) * deviation
    if len(cuts) > 0:
        drawn = shard_levels(rng, shape, cuts, -0.22, 0.18) * drawn
    return jnp.clip(drawn, min=-reach, max=reach).astype(kind)


def setup_inputs(seed: int = 0) -> dict:
    arg_keys = jax.random.split(jax.random.key(seed), 6)
    object_slices = centred(arg_keys[0], (SLICES, 2, ROWS, COLS), 0.7, 2.5, ((2, 16), (3, 16)), jnp.float32)
    probe_wave = centred(arg_keys[1], (2, PROBE, PROBE), 0.7, 4.0, (), jnp.float32)
    offsets = with_ends(jax.random.randint(arg_keys[2], (N_ROW, N_COL, POS, 2), 0, TILE), jax.random.fold_in(arg_keys[2], 1), 0, TILE - 1).astype(jnp.int32)
    active_flags = with_ends((jax.random.randint(arg_keys[3], (N_ROW, N_COL, POS), 0, 4) < 3).astype(jnp.int32), jax.random.fold_in(arg_keys[3], 1), 0, 1)
    intensity = jnp.clip(jnp.exp(math.log(3.0) - 3.4011974 * jax.random.uniform(arg_keys[4], (N_ROW, N_COL, POS, PROBE, PROBE), jnp.float32) ** shard_levels(arg_keys[4], (N_ROW, N_COL, POS, PROBE, PROBE), ((0, 16), (1, 16)), -0.2, 0.2)), 0.1, 3.0)
    return {"object_slices": object_slices, "probe_wave": probe_wave, "offsets": offsets, "active_flags": active_flags, "intensity": intensity}


fresnel_phase = 40.0
object_step = 0.25

def transfer(extent):
    indices = jnp.arange(extent, dtype=jnp.int32)
    frequency = ((indices + extent // 2) % extent - extent // 2).astype(jnp.float32) / extent
    phase_angle = -jnp.pi * fresnel_phase * (frequency[:, None] ** 2 + frequency[None, :] ** 2)
    return (jnp.cos(phase_angle), jnp.sin(phase_angle))

def position_grads(windows, probe_wave, pattern, flag_value, kernel):
    kernel_c = lax.complex(kernel[0], kernel[1])
    transmit = lax.complex(windows[:, 0], windows[:, 1])
    wavefield = lax.complex(probe_wave[0], probe_wave[1])
    incident = []
    exited = wavefield
    for layer_at in range(SLICES):
        incident.append(wavefield)
        exited = wavefield * transmit[layer_at]
        if layer_at + 1 < SLICES:
            wavefield = jnp.fft.ifft2(kernel_c * jnp.fft.fft2(exited, norm='ortho'), norm='ortho')
    far_field = jnp.fft.fft2(exited, norm='ortho')
    excess = flag_value * (jnp.real(far_field) ** 2 + jnp.imag(far_field) ** 2 - pattern)
    back_field = jnp.fft.ifft2(excess * far_field, norm='ortho')
    gradients = [None] * SLICES
    for layer_at in reversed(range(SLICES)):
        gradients[layer_at] = jnp.conj(incident[layer_at]) * back_field
        back_field = jnp.conj(transmit[layer_at]) * back_field
        if layer_at > 0:
            back_field = jnp.fft.ifft2(jnp.conj(kernel_c) * jnp.fft.fft2(back_field, norm='ortho'), norm='ortho')
    grad_window = jnp.stack([jnp.stack([jnp.real(grad_item), jnp.imag(grad_item)]) for grad_item in gradients])
    grad_wave = jnp.stack([jnp.real(back_field), jnp.imag(back_field)])
    return (grad_window, grad_wave)

def fold_rims(grad_pad, margin):
    inner = grad_pad[:, :, :, margin:-margin]
    inner = inner.at[:, :, :, -margin:].add(grad_pad[:, :, :, :margin])
    inner = inner.at[:, :, :, :margin].add(grad_pad[:, :, :, -margin:])
    folded = inner[:, :, margin:-margin]
    folded = folded.at[:, :, -margin:].add(inner[:, :, :margin])
    folded = folded.at[:, :, :margin].add(inner[:, :, -margin:])
    return folded

def reference(object_slices, probe_wave, offsets, active_flags, intensity):
    margin = PROBE // 2
    padded = jnp.pad(object_slices, ((0, 0), (0, 0), (margin, margin), (margin, margin)), mode='wrap')
    kernel = transfer(PROBE)
    tile_rows = jnp.arange(N_ROW, dtype=jnp.int32)[:, None, None] * TILE
    tile_cols = jnp.arange(N_COL, dtype=jnp.int32)[None, :, None] * TILE
    start_rows = (offsets[..., 0] + tile_rows).reshape(-1).astype(jnp.int32)
    start_cols = (offsets[..., 1] + tile_cols).reshape(-1).astype(jnp.int32)
    flag_list = active_flags.reshape(-1)
    observed = intensity.reshape(-1, PROBE, PROBE)

    def accumulate(running, record):
        grad_pad, grad_probe = running
        top_row, left_col, flag_value, pattern = record
        anchor = jnp.zeros((), jnp.int32)
        begin = (anchor, anchor, top_row, left_col)
        windows = lax.dynamic_slice(padded, begin, (SLICES, 2, PROBE, PROBE))
        grad_window, grad_wave = position_grads(windows, probe_wave, pattern, flag_value.astype(jnp.float32), kernel)
        previous = lax.dynamic_slice(grad_pad, begin, (SLICES, 2, PROBE, PROBE))
        grad_pad = lax.dynamic_update_slice(grad_pad, previous + grad_window, begin)
        return ((grad_pad, grad_probe + grad_wave), None)
    initial = (jnp.zeros_like(padded), jnp.zeros_like(probe_wave))
    (grad_pad, grad_probe), _ = lax.scan(accumulate, initial, (start_rows, start_cols, flag_list, observed))
    object_gradient = fold_rims(grad_pad, margin)
    updated_object = object_slices - object_step * object_gradient
    updated_probe = probe_wave - grad_probe * (1.0 / math.sqrt(POS * N_ROW * N_COL))
    return (updated_object, updated_probe)
```

```python
import functools
import math

import jax
import jax.numpy as jnp
import numpy as np
from jax import lax
from jax.experimental import pallas as pl
from jax.experimental.pallas import tpu as pltpu
from jax.sharding import PartitionSpec as P

fresnel_phase = 40.0
object_step = 0.25
N = 128
T = 256
M = 64
S = 4
B = 4
F32 = jnp.float32
BF16 = jnp.bfloat16
MESH = pl.DeviceIdType.MESH


def block_pair(mat):
    re, im = mat.real, mat.imag
    right = np.block([[re, im], [-im, re]])
    left = np.block([[re, -im], [im, re]])
    out = []
    for block in (right, left):
        high = block.astype(np.float32).astype(BF16)
        low = (block - high.astype(np.float64)).astype(np.float32).astype(BF16)
        out += [high, low]
    return np.stack(out)


def tables():
    index = np.arange(N)
    dft = np.exp(-2j * np.pi * (index[:, None] * index[None, :] % N) / N) / math.sqrt(N)
    freq = ((index + N // 2) % N - N // 2) / N
    chirp = np.exp(-1j * np.pi * fresnel_phase * freq**2)
    hop = np.conj(dft) @ (chirp[:, None] * dft)
    return np.stack([block_pair(hop), block_pair(dft)])


def split(x):
    high = x.astype(BF16)
    return high, (x - high.astype(F32)).astype(BF16)


def dot(a, b):
    return jnp.dot(a, b, preferred_element_type=F32)


def both_sides(xr, xi, tab, which, conj):
    r, l = (2, 0) if conj else (0, 2)
    xh, xl = split(jnp.concatenate([xr, xi], axis=1))
    wh, wl = tab[which, r], tab[which, r + 1]
    y = dot(xh, wh) + (dot(xl, wh) + dot(xh, wl))
    cols = []
    for p in range(B):
        part = y[p * N : (p + 1) * N]
        cols.append(jnp.concatenate([part[:, :N], part[:, N:]], axis=0))
    yh, yl = split(jnp.concatenate(cols, axis=1))
    vh, vl = tab[which, l], tab[which, l + 1]
    z = dot(vh, yh) + (dot(vh, yl) + dot(vl, yh))
    zr = jnp.concatenate([z[:N, p * N : (p + 1) * N] for p in range(B)], axis=0)
    zi = jnp.concatenate([z[N:, p * N : (p + 1) * N] for p in range(B)], axis=0)
    return zr, zi


def kernel(
    n_row, n_col,
    offs, flags, obj_hbm, probe, inten, tab,
    out_obj, out_probe,
    tile, pad0, pad1, pad2, pad3, halo, sbuf, wins, psi, zbuf, gpad, rbuf, cbuf, cgot,
    pgrad, ar1, ar2, part1, part2, total,
    obj_sem, hs, hr, ps, pr, rs, rr, cs, cr, as_, ar_,
):
    pads = (pad0, pad1, pad2, pad3)
    me_r = lax.axis_index("row")
    me_c = lax.axis_index("col")
    up, down = lax.rem(me_r + n_row - 1, n_row), lax.rem(me_r + 1, n_row)
    left, right = lax.rem(me_c + n_col - 1, n_col), lax.rem(me_c + 1, n_col)
    lane = lax.broadcasted_iota(jnp.int32, (T, N), 1)
    low = lane < M

    def swap(x):
        return pltpu.roll(x, M, 1)

    def remote(src, dst, ssem, rsem, dev):
        return pltpu.make_async_remote_copy(
            src_ref=src, dst_ref=dst, send_sem=ssem, recv_sem=rsem, device_id=dev, device_id_type=MESH
        )

    loads = [pltpu.make_async_copy(obj_hbm.at[k], tile.at[k], obj_sem.at[k]) for k in range(S)]
    for c in loads:
        c.start()
    barrier = pltpu.get_barrier_semaphore()
    for d in range(1, n_row):
        pl.semaphore_signal(barrier, inc=1, device_id=(lax.rem(me_r + d, n_row), me_c), device_id_type=MESH)
    for d in range(1, n_col):
        pl.semaphore_signal(barrier, inc=1, device_id=(me_r, lax.rem(me_c + d, n_col)), device_id_type=MESH)
    pl.semaphore_wait(barrier, n_row + n_col - 2)

    sends = []
    rim = []
    for k in range(S):
        loads[k].wait()
        re, im = tile[k, 0], tile[k, 1]
        sbuf[k, 0] = jnp.where(low, re[:, :N], swap(im[:, :N]))
        sbuf[k, 1] = jnp.where(low, swap(re[:, N:]), im[:, N:])
        pair = (
            remote(sbuf.at[k, 0], halo.at[k, 1], hs.at[k, 0], hr.at[k, 1], (me_r, left)),
            remote(sbuf.at[k, 1], halo.at[k, 0], hs.at[k, 1], hr.at[k, 0], (me_r, right)),
        )
        for c in pair:
            c.start()
        sends += pair
        rim.append(pair)

    def row_rims(k, j):
        pad = pads[k]
        pair = (
            remote(pad.at[:, j, pl.ds(M, M)], pad.at[:, j, pl.ds(M + T, M)],
                   ps.at[k, j, 0], pr.at[k, j, 1], (up, me_c)),
            remote(pad.at[:, j, pl.ds(T, M)], pad.at[:, j, pl.ds(0, M)],
                   ps.at[k, j, 1], pr.at[k, j, 0], (down, me_c)),
        )
        for c in pair:
            c.start()
        sends.extend(pair)
        return pair

    rows = {k: [] for k in range(S)}
    for k in range(S):
        for ch in range(2):
            pads[k][ch, 1, M : M + T] = jnp.where(low, swap(tile[k, ch, :, :N]), swap(tile[k, ch, :, N:]))
        rows[k] += row_rims(k, 1)

    def clear(i, carry):
        zbuf[i] = jnp.zeros(zbuf.shape[1:], F32)
        return carry

    lax.fori_loop(0, zbuf.shape[0], clear, 0)

    def merge(k):
        for c in rim[k]:
            c.wait_recv()
        lo, hi = halo[k, 0], halo[k, 1]
        pads[k][0, 0, M : M + T] = jnp.where(low, lo, swap(tile[k, 0, :, :N]))
        pads[k][1, 0, M : M + T] = jnp.where(low, swap(lo), swap(tile[k, 1, :, :N]))
        pads[k][0, 2, M : M + T] = jnp.where(low, swap(tile[k, 0, :, N:]), swap(hi))
        pads[k][1, 2, M : M + T] = jnp.where(low, swap(tile[k, 1, :, N:]), hi)
        rows[k] += row_rims(k, 0)
        rows[k] += row_rims(k, 2)

    lane_n = lax.broadcasted_iota(jnp.int32, (N, N), 1)
    spots = []
    for p in range(B):
        sy, sx = offs[2 * p], offs[2 * p + 1]
        spots.append((sy, lax.shift_right_logical(sx, 7), lax.bitwise_and(sx, N - 1)))

    def windows(k):
        for c in rows[k]:
            c.wait_recv()
        for p in range(B):
            sy, q, r = spots[p]
            back = lax.bitwise_and(N - r, N - 1)
            for ch in range(2):
                a = pltpu.roll(pads[k][ch, q, pl.ds(sy, N), :], back, 1)
                b = pltpu.roll(pads[k][ch, q + 1, pl.ds(sy, N), :], back, 1)
                wins[k, ch, p * N : (p + 1) * N] = jnp.where(lane_n < N - r, a, b)

    def incident(k):
        if k == 0:
            return tuple(jnp.concatenate([probe[c]] * B, axis=0) for c in range(2))
        return psi[k - 1, 0], psi[k - 1, 1]

    def exit_wave(k):
        ar, ai = incident(k)
        wr, wi = wins[k, 0], wins[k, 1]
        return ar * wr - ai * wi, ar * wi + ai * wr

    def forward(k):
        zr, zi = both_sides(*exit_wave(k), tab, 0, False)
        psi[k, 0] = zr
        psi[k, 1] = zi

    merge(0)
    for k in range(1, S):
        merge(k)
        windows(k - 1)
        forward(k - 1)
    windows(S - 1)

    fr, fi = both_sides(*exit_wave(S - 1), tab, 1, False)
    level = jnp.concatenate([jnp.full((N, N), flags[p].astype(F32), F32) for p in range(B)], axis=0)
    excess = level * (fr * fr + fi * fi - inten[...])
    gr, gi = both_sides(excess * fr, excess * fi, tab, 1, True)

    def deposit(k, gr, gi):
        ar, ai = incident(k)
        for ch, g in enumerate((ar * gr + ai * gi, ar * gi - ai * gr)):
            for p in range(B):
                r = spots[p][2]
                g_p = pltpu.roll(g[p * N : (p + 1) * N], r, 1)
                zbuf[p * 2 + ch, 1, T : T + N] = jnp.where(lane_n >= r, g_p, 0.0)
                zbuf[p * 2 + ch, 2, T : T + N] = jnp.where(lane_n < r, g_p, 0.0)
        for ch in range(2):
            for j in range(3):
                acc = None
                for p in range(B):
                    sy, q, r = spots[p]
                    group = lax.rem(j + 1 - q + 3, 3)
                    piece = zbuf[p * 2 + ch, group, pl.ds(T - sy, T + N), :]
                    acc = piece if acc is None else acc + piece
                gpad[k, ch, j] = acc
        pair = (
            remote(gpad.at[k, :, :, pl.ds(0, M)], rbuf.at[k, 1], rs.at[k, 0], rr.at[k, 1], (up, me_c)),
            remote(gpad.at[k, :, :, pl.ds(M + T, M)], rbuf.at[k, 0], rs.at[k, 1], rr.at[k, 0], (down, me_c)),
        )
        for c in pair:
            c.start()
        sends.extend(pair)
        return pair

    def fold_rows(k, pair):
        for c in pair:
            c.wait_recv()
        gpad[k, :, :, M : 2 * M] += rbuf[k, 0]
        gpad[k, :, :, T : T + M] += rbuf[k, 1]
        body = slice(M, M + T)
        cbuf[k, 0] = jnp.where(low, gpad[k, 0, 0, body], swap(gpad[k, 1, 0, body]))
        cbuf[k, 1] = jnp.where(low, swap(gpad[k, 0, 2, body]), gpad[k, 1, 2, body])
        cols = (
            remote(cbuf.at[k, 0], cgot.at[k, 1], cs.at[k, 0], cr.at[k, 1], (me_r, left)),
            remote(cbuf.at[k, 1], cgot.at[k, 0], cs.at[k, 1], cr.at[k, 0], (me_r, right)),
        )
        for c in cols:
            c.start()
        sends.extend(cols)
        return cols

    cols = {}
    for k in range(S - 1, -1, -1):
        pair = deposit(k, gr, gi)
        wr, wi = wins[k, 0], wins[k, 1]
        gr, gi = wr * gr + wi * gi, wr * gi - wi * gr
        if k > 0:
            gr, gi = both_sides(gr, gi, tab, 0, True)
        else:
            for c, g in enumerate((gr, gi)):
                pgrad[c * N : (c + 1) * N] = (g[:N] + g[N : 2 * N]) + (g[2 * N : 3 * N] + g[3 * N :])
        cols[k] = fold_rows(k, pair)

    depth = 2 * N // n_row

    def exchange(stage, axis, pick_src, pick_dst):
        count = n_row if axis == 0 else n_col
        me = me_r if axis == 0 else me_c
        out = []
        for d in range(1, count):
            peer = lax.rem(me + d, count)
            dev = (peer, me_c) if axis == 0 else (me_r, peer)
            out.append(remote(pick_src(peer), pick_dst(me), as_.at[stage, d], ar_.at[stage, d], dev))
        for c in out:
            c.start()
        sends.extend(out)
        return out

    def rows_of(ref, i):
        return ref.at[pl.ds(pl.multiple_of(i * depth, 8), depth)]

    own = pl.ds(pl.multiple_of(me_r * depth, 8), depth)
    flow = exchange(0, 0, lambda i: rows_of(pgrad, i), lambda me: ar1.at[me])
    ar1[me_r] = pgrad[own, :]
    for c in flow:
        c.wait_recv()
    acc = ar1[0]
    for i in range(1, n_row):
        acc = acc + ar1[i]
    part1[...] = acc
    flow = exchange(1, 1, lambda i: part1, lambda me: ar2.at[me])
    ar2[me_c] = acc
    for c in flow:
        c.wait_recv()
    acc = ar2[0]
    for i in range(1, n_col):
        acc = acc + ar2[i]
    part2[...] = acc
    flow = exchange(2, 0, lambda i: part2, lambda me: rows_of(total, me))
    total[own, :] = acc
    for c in flow:
        c.wait_recv()
    factor = 1.0 / math.sqrt(B * n_row * n_col)
    for c in range(2):
        out_probe[c] = probe[c] - factor * total[c * N : (c + 1) * N]

    body = slice(M, M + T)
    for k in range(S - 1, -1, -1):
        for c in cols[k]:
            c.wait_recv()
        lo, hi = cgot[k, 0], cgot[k, 1]
        for ch in range(2):
            t0, t1, t2 = (swap(gpad[k, ch, j, body]) for j in range(3))
            lo_c, hi_c = (lo, swap(hi)) if ch == 0 else (swap(lo), hi)
            out_obj[k, ch, :, :N] = tile[k, ch, :, :N] - object_step * jnp.where(low, t0 + lo_c, t1)
            out_obj[k, ch, :, N:] = tile[k, ch, :, N:] - object_step * jnp.where(low, t1, t2 + hi_c)
    for c in sends:
        c.wait_send()


def body(n_row, n_col, object_slices, probe_wave, offsets, active_flags, intensity):
    depth = 2 * N // n_row
    vmem = pl.BlockSpec(memory_space=pltpu.VMEM)
    smem = pl.BlockSpec(memory_space=pltpu.SMEM)
    dma = pltpu.SemaphoreType.DMA
    scratch = (
        [pltpu.VMEM((S, 2, T, T), F32)]
        + [pltpu.VMEM((2, 3, T + N, N), F32)] * S
        + [
            pltpu.VMEM((S, 2, T, N), F32),
            pltpu.VMEM((S, 2, T, N), F32),
            pltpu.VMEM((S, 2, B * N, N), F32),
            pltpu.VMEM((S - 1, 2, B * N, N), F32),
            pltpu.VMEM((2 * B, 3, 2 * T + N, N), F32),
            pltpu.VMEM((S, 2, 3, T + N, N), F32),
            pltpu.VMEM((S, 2, 2, 3, M, N), F32),
            pltpu.VMEM((S, 2, T, N), F32),
            pltpu.VMEM((S, 2, T, N), F32),
            pltpu.VMEM((2 * N, N), F32),
            pltpu.VMEM((n_row, depth, N), F32),
            pltpu.VMEM((n_col, depth, N), F32),
            pltpu.VMEM((depth, N), F32),
            pltpu.VMEM((depth, N), F32),
            pltpu.VMEM((2 * N, N), F32),
        ]
        + [dma((S,)), dma((S, 2)), dma((S, 2)), dma((S, 3, 2)), dma((S, 3, 2))]
        + [dma((S, 2)), dma((S, 2)), dma((S, 2)), dma((S, 2))]
        + [dma((3, max(n_row, n_col))), dma((3, max(n_row, n_col)))]
    )
    return pl.pallas_call(
        functools.partial(kernel, n_row, n_col),
        out_shape=(
            jax.ShapeDtypeStruct((S, 2, T, T), F32),
            jax.ShapeDtypeStruct((2, N, N), F32),
        ),
        in_specs=[smem, smem, pl.BlockSpec(memory_space=pl.ANY), vmem, vmem, vmem],
        out_specs=(vmem, vmem),
        scratch_shapes=scratch,
        compiler_params=pltpu.CompilerParams(
            collective_id=0, has_side_effects=True, vmem_limit_bytes=60000000
        ),
        name="step",
    )(
        offsets.reshape(2 * B),
        active_flags.reshape(B),
        object_slices,
        probe_wave,
        intensity.reshape(B * N, N),
        jnp.asarray(tables()),
    )


def solution(mesh):
    in_specs = (
        P(None, None, "row", "col"),
        P(),
        P("row", "col", None, None),
        P("row", "col", None),
        P("row", "col", None, None, None),
    )
    out_specs = (P(None, None, "row", "col"), P())
    run = functools.partial(body, mesh.shape["row"], mesh.shape["col"])
    return jax.shard_map(run, mesh=mesh, in_specs=in_specs, out_specs=out_specs, check_vma=False)
```

```python
import functools
import math

import jax
import jax.numpy as jnp
import numpy as np
from jax import lax
from jax.experimental import pallas as pl
from jax.experimental.pallas import tpu as pltpu
from jax.sharding import PartitionSpec as P

fresnel_phase = 40.0
object_step = 0.25
N = 128
T = 256
M = 64
S = 4
B = 4
G1, YY, ZH = 8, 4, 4
VMEM_LIMIT = 52000000
F32 = jnp.float32
BF16 = jnp.bfloat16
MESH = pl.DeviceIdType.MESH


def block_pair(mat):
    re, im = mat.real, mat.imag
    right = np.block([[re, im], [-im, re]])
    left = np.block([[re, -im], [im, re]])
    out = []
    for block in (right, left):
        high = block.astype(np.float32).astype(BF16)
        low = (block - high.astype(np.float64)).astype(np.float32).astype(BF16)
        out += [high, low]
    return np.stack(out)


def tables():
    index = np.arange(N)
    dft = np.exp(-2j * np.pi * (index[:, None] * index[None, :] % N) / N) / math.sqrt(N)
    freq = ((index + N // 2) % N - N // 2) / N
    chirp = np.exp(-1j * np.pi * fresnel_phase * freq**2)
    hop = np.conj(dft) @ (chirp[:, None] * dft)
    return np.stack([block_pair(hop), block_pair(dft)])


def split(x):
    high = x.astype(BF16)
    return high, (x - high.astype(F32)).astype(BF16)


def dot(a, b):
    return jnp.dot(a, b, preferred_element_type=F32)


def both_sides(xr, xi, tab, which, conj):
    r, l = (2, 0) if conj else (0, 2)
    xh, xl = split(jnp.concatenate([xr, xi], axis=1))
    wh, wl = tab[which, r], tab[which, r + 1]
    y = dot(xh, wh) + (dot(xl, wh) + dot(xh, wl))
    cols = []
    for p in range(B):
        part = y[p * N : (p + 1) * N]
        cols.append(jnp.concatenate([part[:, :N], part[:, N:]], axis=0))
    yh, yl = split(jnp.concatenate(cols, axis=1))
    vh, vl = tab[which, l], tab[which, l + 1]
    z = dot(vh, yh) + (dot(vh, yl) + dot(vl, yh))
    zr = jnp.concatenate([z[:N, p * N : (p + 1) * N] for p in range(B)], axis=0)
    zi = jnp.concatenate([z[N:, p * N : (p + 1) * N] for p in range(B)], axis=0)
    return zr, zi


def kernel(
    n_row, n_col,
    offs, flags, obj_hbm, probe_hbm, inten_hbm, tab_hbm,
    out_obj, out_probe,
    tile, probe, inten, tab, pad0, pad1, pad2, pad3, halo, sbuf, wins, psi, zbuf, gpad, rbuf, cbuf, cgot,
    pgrad, ar1, ar2, ar3, part1, part2, part3, part4, total,
    obj_sem, in_sem, out_sem, sent, hr, pr, rr, cr, got,
):
    pads = (pad0, pad1, pad2, pad3)
    me_r = lax.axis_index("row")
    me_c = lax.axis_index("col")
    up, down = lax.rem(me_r + n_row - 1, n_row), lax.rem(me_r + 1, n_row)
    left, right = lax.rem(me_c + n_col - 1, n_col), lax.rem(me_c + 1, n_col)
    zl, j1 = lax.div(me_r, G1), lax.rem(me_r, G1)
    yy, zh = lax.div(me_c, ZH), lax.rem(me_c, ZH)
    group1 = [lax.rem(j1 + d, G1) for d in range(1, G1)]
    group2 = [lax.rem(yy + d, YY) for d in range(1, YY)]
    group3 = [(lax.rem(zl + a, 2), lax.rem(zh + b, ZH)) for a in range(2) for b in range(ZH) if a or b]
    low = lax.broadcasted_iota(jnp.int32, (T, N), 1) < M

    def low_of(x):
        return low[: x.shape[0]]

    def swap(x):
        return pltpu.roll(x, M, 1)

    def remote(src, dst, ssem, rsem, dev):
        return pltpu.make_async_remote_copy(
            src_ref=src, dst_ref=dst, send_sem=ssem, recv_sem=rsem, device_id=dev, device_id_type=MESH
        )

    loads = [pltpu.make_async_copy(obj_hbm.at[k], tile.at[k], obj_sem.at[k]) for k in range(S)]
    for c in loads:
        c.start()
    others = [
        pltpu.make_async_copy(a, b, in_sem.at[i])
        for i, (a, b) in enumerate(((probe_hbm, probe), (tab_hbm, tab), (inten_hbm, inten)))
    ]
    for c in others:
        c.start()
    barrier = pltpu.get_barrier_semaphore()
    greet = [(up, me_c), (down, me_c), (me_r, left), (me_r, right)]
    greet += [(zl * G1 + j, me_c) for j in group1]
    greet += [(me_r, y * ZH + zh) for y in group2]
    greet += [(a * G1 + j1, yy * ZH + b) for a, b in group3]
    for dev in greet:
        pl.semaphore_signal(barrier, inc=1, device_id=dev, device_id_type=MESH)

    def go(*copies):
        for c in copies:
            c.start()

    def drain(ref, sem):
        pltpu.make_async_copy(ref, ref, sem).wait()

    PARTS = (slice(0, N), slice(N, T))
    ROWS = (((slice(0, M), slice(0, M)), (slice(M, N), slice(T - M, T))), ((slice(N, T), slice(M, T - M)),))

    def pack(k):
        loads[k].wait()
        for ds, ts in ROWS[0] + ROWS[1]:
            r0, r1 = tile[k, 0, ts, :N], tile[k, 0, ts, N:]
            i0, i1 = tile[k, 1, ts, :N], tile[k, 1, ts, N:]
            m = low_of(r0)
            sbuf[k, 0, ds] = jnp.where(m, r0, swap(i0))
            sbuf[k, 1, ds] = jnp.where(m, swap(r1), i1)
            rows = slice(M + ts.start, M + ts.stop)
            pads[k][0, 2, rows] = jnp.where(m, swap(r0), swap(r1))
            pads[k][1, 2, rows] = jnp.where(m, swap(i0), swap(i1))

    def send_rim(k, part):
        rows = pl.ds(part * N, N)
        go(
            remote(sbuf.at[k, 0, rows], halo.at[k, 1, rows], sent.at[0], hr.at[k, part], (me_r, left)),
            remote(sbuf.at[k, 1, rows], halo.at[k, 0, rows], sent.at[0], hr.at[k, part], (me_r, right)),
        )

    def send_rows(k, j, n):
        pad, js = pads[k], pl.ds(j, n)
        go(
            remote(pad.at[:, js, pl.ds(M, M)], pad.at[:, js, pl.ds(M + T, M)], sent.at[1], pr.at[k], (up, me_c)),
            remote(pad.at[:, js, pl.ds(T, M)], pad.at[:, js, pl.ds(0, M)], sent.at[1], pr.at[k], (down, me_c)),
        )

    def merge(k, part):
        drain(halo.at[k, :, pl.ds(part * N, N)], hr.at[k, part])
        for ds, ts in ROWS[part]:
            lo, hi = halo[k, 0, ds], halo[k, 1, ds]
            m = low_of(lo)
            rows = slice(M + ts.start, M + ts.stop)
            pads[k][0, 0, rows] = jnp.where(m, lo, swap(tile[k, 0, ts, :N]))
            pads[k][1, 0, rows] = jnp.where(m, swap(lo), swap(tile[k, 1, ts, :N]))
            pads[k][0, 1, rows] = jnp.where(m, swap(tile[k, 0, ts, N:]), swap(hi))
            pads[k][1, 1, rows] = jnp.where(m, swap(tile[k, 1, ts, N:]), hi)
        if part == 0:
            send_rows(k, 0, 2)

    lane_n = lax.broadcasted_iota(jnp.int32, (N, N), 1)
    spots = []
    for p in range(B):
        sy, sx = offs[0, p], offs[1, p]
        spots.append((sy, lax.shift_right_logical(sx, 7), lax.bitwise_and(sx, N - 1)))

    def windows(k):
        drain(rbuf.at[k], pr.at[k])
        for p in range(B):
            sy, q, r = spots[p]
            back = lax.bitwise_and(N - r, N - 1)
            for ch in range(2):
                a = pltpu.roll(pads[k][ch, 2 * q, pl.ds(sy, N), :], back, 1)
                b = pltpu.roll(pads[k][ch, 2 - q, pl.ds(sy, N), :], back, 1)
                wins[k, ch, p * N : (p + 1) * N] = jnp.where(lane_n < N - r, a, b)

    def incident(k):
        if k == 0:
            return tuple(jnp.concatenate([probe[c]] * B, axis=0) for c in range(2))
        return psi[k - 1, 0], psi[k - 1, 1]

    def exit_wave(k):
        ar, ai = incident(k)
        wr, wi = wins[k, 0], wins[k, 1]
        return ar * wr - ai * wi, ar * wi + ai * wr

    def forward(k):
        zr, zi = both_sides(*exit_wave(k), tab, 0, False)
        psi[k, 0] = zr
        psi[k, 1] = zi

    pack(0)
    pl.semaphore_wait(barrier, len(greet))
    send_rim(0, 0)
    send_rows(0, 2, 1)
    pack(1)
    send_rim(1, 0)
    send_rim(0, 1)
    send_rows(1, 2, 1)
    pack(2)
    pack(3)

    def clear(i, carry):
        zbuf[i] = jnp.zeros(zbuf.shape[1:], F32)
        return carry

    lax.fori_loop(0, zbuf.shape[0], clear, 0)
    for c in others:
        c.wait()

    merge(0, 0)
    send_rim(2, 0)
    send_rim(1, 1)
    send_rows(2, 2, 1)
    merge(1, 0)
    send_rim(3, 0)
    send_rim(2, 1)
    send_rows(3, 2, 1)
    merge(0, 1)
    windows(0)
    forward(0)
    merge(2, 0)
    send_rim(3, 1)
    merge(1, 1)
    windows(1)
    forward(1)
    merge(3, 0)
    merge(2, 1)
    windows(2)
    forward(2)
    merge(3, 1)
    windows(3)

    fr, fi = both_sides(*exit_wave(S - 1), tab, 1, False)
    level = jnp.concatenate([jnp.full((N, N), flags[p].astype(F32), F32) for p in range(B)], axis=0)
    excess = level * (fr * fr + fi * fi - inten[...])
    gr, gi = both_sides(excess * fr, excess * fi, tab, 1, True)

    def pack_cols(k, part):
        for ds, ts in ROWS[part]:
            rows = slice(M + ts.start, M + ts.stop)
            m = low_of(gpad[k, 0, 0, rows])
            cbuf[k, 0, ds] = jnp.where(m, gpad[k, 0, 0, rows], swap(gpad[k, 1, 0, rows]))
            cbuf[k, 1, ds] = jnp.where(m, swap(gpad[k, 0, 2, rows]), gpad[k, 1, 2, rows])
        rows = pl.ds(part * N, N)
        go(
            remote(cbuf.at[k, 0, rows], cgot.at[k, 1, rows], sent.at[2], cr.at[k, part], (me_r, left)),
            remote(cbuf.at[k, 1, rows], cgot.at[k, 0, rows], sent.at[2], cr.at[k, part], (me_r, right)),
        )

    def deposit(k, gr, gi):
        ar, ai = incident(k)
        for ch, g in enumerate((ar * gr + ai * gi, ar * gi - ai * gr)):
            for p in range(B):
                r = spots[p][2]
                g_p = pltpu.roll(g[p * N : (p + 1) * N], r, 1)
                zbuf[p * 2 + ch, 1, T : T + N] = jnp.where(lane_n >= r, g_p, 0.0)
                zbuf[p * 2 + ch, 2, T : T + N] = jnp.where(lane_n < r, g_p, 0.0)
        for ch in range(2):
            for j in range(3):
                acc = None
                for p in range(B):
                    sy, q, r = spots[p]
                    group = lax.rem(j + 1 - q + 3, 3)
                    piece = zbuf[p * 2 + ch, group, pl.ds(T - sy, T + N), :]
                    acc = piece if acc is None else acc + piece
                gpad[k, ch, j] = acc
        go(
            remote(gpad.at[k, :, :, pl.ds(0, M)], rbuf.at[k, 1], sent.at[3], rr.at[k], (up, me_c)),
            remote(gpad.at[k, :, :, pl.ds(M + T, M)], rbuf.at[k, 0], sent.at[3], rr.at[k], (down, me_c)),
        )
        pack_cols(k, 1)

    def fold_rows(k):
        drain(rbuf.at[k], rr.at[k])
        gpad[k, :, :, M : 2 * M] += rbuf[k, 0]
        gpad[k, :, :, T : T + M] += rbuf[k, 1]
        pack_cols(k, 0)

    for k in range(S - 1, -1, -1):
        deposit(k, gr, gi)
        wr, wi = wins[k, 0], wins[k, 1]
        gr, gi = wr * gr + wi * gi, wr * gi - wi * gr
        if k > 0:
            gr, gi = both_sides(gr, gi, tab, 0, True)
    for c, g in enumerate((gr, gi)):
        pgrad[c * N : (c + 1) * N] = (g[:N] + g[N : 2 * N]) + (g[2 * N : 3 * N] + g[3 * N :])

    D1 = 2 * N // G1
    D2 = D1 // YY

    def at(ref, i, depth):
        return ref.at[pl.ds(pl.multiple_of(i * depth, 8), depth)]

    def sum_of(ref):
        acc = ref[0]
        for i in range(1, ref.shape[0]):
            acc = acc + ref[i]
        return acc

    def arrive(stage, ref):
        drain(ref.at[pl.ds(0, ref.shape[0] - ref.shape[0] // COUNT[stage])], got.at[stage])

    COUNT = (G1, YY, 2 * ZH, YY, G1)
    go(*[
        remote(at(pgrad, j, D1), ar1.at[j1], sent.at[4], got.at[0], (zl * G1 + j, me_c))
        for j in group1
    ])
    ar1[j1] = pgrad[pl.ds(pl.multiple_of(j1 * D1, 8), D1), :]
    arrive(0, ar1)
    part1[...] = sum_of(ar1)
    go(*[
        remote(at(part1, y, D2), ar2.at[yy], sent.at[5], got.at[1], (me_r, y * ZH + zh))
        for y in group2
    ])
    ar2[yy] = part1[pl.ds(pl.multiple_of(yy * D2, 8), D2), :]
    arrive(1, ar2)
    zz = zh * 2 + zl
    acc = sum_of(ar2)
    part2[...] = acc
    ar3[zz] = acc
    go(*[
        remote(part2, ar3.at[zz], sent.at[6], got.at[2], (a * G1 + j1, yy * ZH + b))
        for a, b in group3
    ])
    fold_rows(3)
    fold_rows(2)
    fold_rows(1)
    fold_rows(0)

    def finish(k):
        for part in range(2):
            drain(cgot.at[k, :, pl.ds(part * N, N)], cr.at[k, part])
            for ds, ts in ROWS[part]:
                lo, hi = cgot[k, 0, ds], cgot[k, 1, ds]
                rows = slice(M + ts.start, M + ts.stop)
                m = low_of(lo)
                for ch in range(2):
                    t0, t1, t2 = (swap(gpad[k, ch, j, rows]) for j in range(3))
                    lo_c, hi_c = (lo, swap(hi)) if ch == 0 else (swap(lo), hi)
                    tile[k, ch, ts, :N] -= object_step * jnp.where(m, t0 + lo_c, t1)
                    tile[k, ch, ts, N:] -= object_step * jnp.where(m, t1, t2 + hi_c)
        c = pltpu.make_async_copy(tile.at[k], out_obj.at[k], out_sem.at[k])
        c.start()
        return c

    arrive(2, ar3)
    acc = sum_of(ar3)
    part3[...] = acc
    part4[pl.ds(pl.multiple_of(yy * D2, 8), D2), :] = acc
    go(*[
        remote(part3, at(part4, yy, D2), sent.at[7], got.at[3], (me_r, y * ZH + zh))
        for y in group2
    ])
    arrive(3, part4)
    go(*[
        remote(part4, at(total, j1, D1), sent.at[8], got.at[4], (zl * G1 + j, me_c))
        for j in group1
    ])
    total[pl.ds(pl.multiple_of(j1 * D1, 8), D1), :] = part4[...]
    stores = [finish(3), finish(2)]
    arrive(4, total)
    factor = 1.0 / math.sqrt(B * n_row * n_col)
    for c in range(2):
        out_probe[c] = probe[c] - factor * total[c * N : (c + 1) * N]
    stores += [finish(1), finish(0)]
    drain(sbuf, sent.at[0])
    drain(rbuf, sent.at[1])
    drain(cbuf, sent.at[2])
    drain(rbuf, sent.at[3])
    for stage, ref in enumerate((ar1, ar2, ar3, part4, total)):
        drain(ref.at[pl.ds(0, ref.shape[0] - ref.shape[0] // COUNT[stage])], sent.at[4 + stage])
    for c in stores:
        c.wait()


def body(n_row, n_col, object_slices, probe_wave, offsets, active_flags, intensity):
    vmem = pl.BlockSpec(memory_space=pltpu.VMEM)
    smem = pl.BlockSpec(memory_space=pltpu.SMEM)
    hbm = pl.BlockSpec(memory_space=pltpu.HBM)
    dma = pltpu.SemaphoreType.DMA

    def stay(x):
        return pltpu.with_memory_space_constraint(x, pltpu.HBM)

    scratch = (
        [
            pltpu.VMEM((S, 2, T, T), F32),
            pltpu.VMEM((2, N, N), F32),
            pltpu.VMEM((B * N, N), F32),
            pltpu.VMEM((2, 4, 2 * N, 2 * N), BF16),
        ]
        + [pltpu.VMEM((2, 3, T + N, N), F32)] * S
        + [
            pltpu.VMEM((S, 2, T, N), F32),
            pltpu.VMEM((S, 2, T, N), F32),
            pltpu.VMEM((S, 2, B * N, N), F32),
            pltpu.VMEM((S - 1, 2, B * N, N), F32),
            pltpu.VMEM((2 * B, 3, 2 * T + N, N), F32),
            pltpu.VMEM((S, 2, 3, T + N, N), F32),
            pltpu.VMEM((S, 2, 2, 3, M, N), F32),
            pltpu.VMEM((S, 2, T, N), F32),
            pltpu.VMEM((S, 2, T, N), F32),
            pltpu.VMEM((2 * N, N), F32),
            pltpu.VMEM((G1, 2 * N // G1, N), F32),
            pltpu.VMEM((YY, 8, N), F32),
            pltpu.VMEM((2 * ZH, 8, N), F32),
            pltpu.VMEM((2 * N // G1, N), F32),
            pltpu.VMEM((8, N), F32),
            pltpu.VMEM((8, N), F32),
            pltpu.VMEM((2 * N // G1, N), F32),
            pltpu.VMEM((2 * N, N), F32),
        ]
        + [dma((S,)), dma((3,)), dma((S,)), dma((9,))]
        + [dma((S, 2)), dma((S,)), dma((S,)), dma((S, 2)), dma((5,))]
    )
    return pl.pallas_call(
        functools.partial(kernel, n_row, n_col),
        out_shape=(
            jax.ShapeDtypeStruct((S, 2, T, T), F32),
            jax.ShapeDtypeStruct((2, N, N), F32),
        ),
        in_specs=[smem, smem, hbm, hbm, hbm, hbm],
        out_specs=(pl.BlockSpec(memory_space=pl.ANY), vmem),
        scratch_shapes=scratch,
        compiler_params=pltpu.CompilerParams(
            collective_id=0, has_side_effects=True, vmem_limit_bytes=VMEM_LIMIT
        ),
        name="step",
    )(
        stay(jnp.transpose(offsets.reshape(B, 2))),
        stay(active_flags.reshape(B)),
        stay(object_slices),
        stay(probe_wave),
        stay(intensity.reshape(B * N, N)),
        stay(jnp.asarray(tables())),
    )


def solution(mesh):
    in_specs = (
        P(None, None, "row", "col"),
        P(),
        P("row", "col", None, None),
        P("row", "col", None),
        P("row", "col", None, None, None),
    )
    out_specs = (P(None, None, "row", "col"), P())
    run = functools.partial(body, mesh.shape["row"], mesh.shape["col"])
    return jax.shard_map(run, mesh=mesh, in_specs=in_specs, out_specs=out_specs, check_vma=False)
```

```python
import functools
import math

import jax
import jax.numpy as jnp
import numpy as np
from jax import lax
from jax.experimental import pallas as pl
from jax.experimental.pallas import tpu as pltpu
from jax.sharding import PartitionSpec as P

fresnel_phase = 40.0
object_step = 0.25
N = 128
T = 256
M = 64
S = 4
B = 4
G1, YY, ZH = 8, 4, 4
RELAY_NEAR = True
VMEM_LIMIT = 52000000
F32 = jnp.float32
BF16 = jnp.bfloat16
MESH = pl.DeviceIdType.MESH


def block_pair(mat):
    re, im = mat.real, mat.imag
    right = np.block([[re, im], [-im, re]])
    left = np.block([[re, -im], [im, re]])
    out = []
    for block in (right, left):
        high = block.astype(np.float32).astype(BF16)
        low = (block - high.astype(np.float64)).astype(np.float32).astype(BF16)
        out += [high, low]
    return np.stack(out)


def tables():
    index = np.arange(N)
    dft = np.exp(-2j * np.pi * (index[:, None] * index[None, :] % N) / N) / math.sqrt(N)
    freq = ((index + N // 2) % N - N // 2) / N
    chirp = np.exp(-1j * np.pi * fresnel_phase * freq**2)
    hop = np.conj(dft) @ (chirp[:, None] * dft)
    return np.stack([block_pair(hop), block_pair(dft)])


def split(x):
    high = x.astype(BF16)
    return high, (x - high.astype(F32)).astype(BF16)


def dot(a, b):
    return jnp.dot(a, b, preferred_element_type=F32)


def both_sides(xr, xi, tab, which, conj):
    r, l = (2, 0) if conj else (0, 2)
    xh, xl = split(jnp.concatenate([xr, xi], axis=1))
    wh, wl = tab[which, r], tab[which, r + 1]
    y = dot(xh, wh) + (dot(xl, wh) + dot(xh, wl))
    cols = []
    for p in range(B):
        part = y[p * N : (p + 1) * N]
        cols.append(jnp.concatenate([part[:, :N], part[:, N:]], axis=0))
    yh, yl = split(jnp.concatenate(cols, axis=1))
    vh, vl = tab[which, l], tab[which, l + 1]
    z = dot(vh, yh) + (dot(vh, yl) + dot(vl, yh))
    zr = jnp.concatenate([z[:N, p * N : (p + 1) * N] for p in range(B)], axis=0)
    zi = jnp.concatenate([z[N:, p * N : (p + 1) * N] for p in range(B)], axis=0)
    return zr, zi


def kernel(
    n_row, n_col,
    offs, flags, obj_hbm, probe_hbm, inten_hbm, tab_hbm,
    out_obj, out_probe,
    tile, probe, inten, tab, pad0, pad1, pad2, pad3, halo, sbuf, wins, psi, zbuf, gpad, rbuf, cbuf, cgot,
    pgrad, ar1, ar2, ar3, part1, part2, part3, part4, total, relay,
    obj_sem, in_sem, out_sem, sent, hr, pr, rr, cr, got, relay_got, relay_sent,
):
    pads = (pad0, pad1, pad2, pad3)
    me_r = lax.axis_index("row")
    me_c = lax.axis_index("col")
    up, down = lax.rem(me_r + n_row - 1, n_row), lax.rem(me_r + 1, n_row)
    left, right = lax.rem(me_c + n_col - 1, n_col), lax.rem(me_c + 1, n_col)
    zl, j1 = lax.div(me_r, G1), lax.rem(me_r, G1)
    yy, zh = lax.div(me_c, ZH), lax.rem(me_c, ZH)
    group1 = [lax.rem(j1 + d, G1) for d in range(1, G1)]
    group2 = [lax.rem(yy + d, YY) for d in range(1, YY)]
    group3 = [(lax.rem(zl + a, 2), lax.rem(zh + b, ZH)) for a in range(2) for b in range(ZH) if a or b]
    low = lax.broadcasted_iota(jnp.int32, (T, N), 1) < M
    zo = 1 - zl
    z_relay, z_final = (zl, zo) if RELAY_NEAR else (zo, zl)
    relay_up, relay_down = z_relay * G1 + 2, z_relay * G1 + G1 - 3
    final_up, final_down = z_final * G1 + G1 - 1, z_final * G1

    def low_of(x):
        return low[: x.shape[0]]

    def swap(x):
        return pltpu.roll(x, M, 1)

    def remote(src, dst, ssem, rsem, dev):
        return pltpu.make_async_remote_copy(
            src_ref=src, dst_ref=dst, send_sem=ssem, recv_sem=rsem, device_id=dev, device_id_type=MESH
        )

    loads = [pltpu.make_async_copy(obj_hbm.at[k], tile.at[k], obj_sem.at[k]) for k in range(S)]
    for c in loads:
        c.start()
    others = [
        pltpu.make_async_copy(a, b, in_sem.at[i])
        for i, (a, b) in enumerate(((probe_hbm, probe), (tab_hbm, tab), (inten_hbm, inten)))
    ]
    for c in others:
        c.start()
    barrier = pltpu.get_barrier_semaphore()
    greet = [(up, me_c), (down, me_c), (me_r, left), (me_r, right)]
    greet += [(zl * G1 + j, me_c) for j in group1]
    greet += [(me_r, y * ZH + zh) for y in group2]
    greet += [(a * G1 + j1, yy * ZH + b) for a, b in group3]
    reach = 3 if RELAY_NEAR else 2
    greet += [(zo * G1 + lax.rem(j1 + d, G1), me_c) for d in (reach, G1 - reach)]
    for dev in greet:
        pl.semaphore_signal(barrier, inc=1, device_id=dev, device_id_type=MESH)

    def go(*copies):
        for c in copies:
            c.start()

    def drain(ref, sem):
        pltpu.make_async_copy(ref, ref, sem).wait()

    PARTS = (slice(0, N), slice(N, T))
    ROWS = (((slice(0, M), slice(0, M)), (slice(M, N), slice(T - M, T))), ((slice(N, T), slice(M, T - M)),))

    def pack(k):
        loads[k].wait()
        for ds, ts in ROWS[0] + ROWS[1]:
            r0, r1 = tile[k, 0, ts, :N], tile[k, 0, ts, N:]
            i0, i1 = tile[k, 1, ts, :N], tile[k, 1, ts, N:]
            m = low_of(r0)
            sbuf[k, 0, ds] = jnp.where(m, r0, swap(i0))
            sbuf[k, 1, ds] = jnp.where(m, swap(r1), i1)
            rows = slice(M + ts.start, M + ts.stop)
            pads[k][0, 2, rows] = jnp.where(m, swap(r0), swap(r1))
            pads[k][1, 2, rows] = jnp.where(m, swap(i0), swap(i1))

    def send_rim(k, part):
        rows = pl.ds(part * N, N)
        go(
            remote(sbuf.at[k, 0, rows], halo.at[k, 1, rows], sent.at[0], hr.at[k, part], (me_r, left)),
            remote(sbuf.at[k, 1, rows], halo.at[k, 0, rows], sent.at[0], hr.at[k, part], (me_r, right)),
        )

    def send_rows(src, top, bottom, ssem, rsem):
        side = pl.ds(0, 2)
        go(
            remote(src.at[:, side, top[0]], top[1].at[:, side], ssem, rsem, (up, me_c)),
            remote(src.at[:, side, bottom[0]], bottom[1].at[:, side], ssem, rsem, (down, me_c)),
        )

    def send_middle(src, top, bottom, ssem, rsem, slot):
        for (rows, dst), edge, dev, hop in (
            (top, j1 == 0, up, relay_up), (bottom, j1 == G1 - 1, down, relay_down)
        ):
            @pl.when(edge)
            def _():
                remote(src.at[:, 2, rows], relay.at[slot], ssem, relay_got.at[slot], (hop, me_c)).start()

            @pl.when(jnp.logical_not(edge))
            def _():
                remote(src.at[:, 2, rows], dst.at[:, 2], ssem, rsem, (dev, me_c)).start()

    def pass_on(top, bottom, rsem, slot):
        for dst, here, dev in ((top, j1 == 2, final_up), (bottom, j1 == G1 - 3, final_down)):
            @pl.when(here)
            def _():
                drain(relay.at[slot], relay_got.at[slot])
                remote(relay.at[slot], dst.at[:, 2], relay_sent, rsem, (dev, me_c)).start()

    def in_top(k):
        return pads[k].at[:, :, pl.ds(M + T, M)]

    def in_bottom(k):
        return pads[k].at[:, :, pl.ds(0, M)]

    def in_args(k):
        return pads[k], (pl.ds(M, M), in_top(k)), (pl.ds(T, M), in_bottom(k)), sent.at[1], pr.at[k]

    def middle_in(k):
        send_middle(*in_args(k), k)

    def relay_in(k):
        pass_on(in_top(k), in_bottom(k), pr.at[k], k)

    def out_args(k):
        return (
            gpad.at[k], (pl.ds(0, M), rbuf.at[k, 1]), (pl.ds(M + T, M), rbuf.at[k, 0]), sent.at[3], rr.at[k]
        )

    def relay_out(k):
        pass_on(rbuf.at[k, 1], rbuf.at[k, 0], rr.at[k], S + k)

    def merge(k, part):
        drain(halo.at[k, :, pl.ds(part * N, N)], hr.at[k, part])
        for ds, ts in ROWS[part]:
            lo, hi = halo[k, 0, ds], halo[k, 1, ds]
            m = low_of(lo)
            rows = slice(M + ts.start, M + ts.stop)
            pads[k][0, 0, rows] = jnp.where(m, lo, swap(tile[k, 0, ts, :N]))
            pads[k][1, 0, rows] = jnp.where(m, swap(lo), swap(tile[k, 1, ts, :N]))
            pads[k][0, 1, rows] = jnp.where(m, swap(tile[k, 0, ts, N:]), swap(hi))
            pads[k][1, 1, rows] = jnp.where(m, swap(tile[k, 1, ts, N:]), hi)
        if part == 0:
            send_rows(*in_args(k))

    lane_n = lax.broadcasted_iota(jnp.int32, (N, N), 1)
    spots = []
    for p in range(B):
        sy, sx = offs[0, p], offs[1, p]
        spots.append((sy, lax.shift_right_logical(sx, 7), lax.bitwise_and(sx, N - 1)))

    def windows(k):
        drain(rbuf.at[k], pr.at[k])
        for p in range(B):
            sy, q, r = spots[p]
            back = lax.bitwise_and(N - r, N - 1)
            for ch in range(2):
                a = pltpu.roll(pads[k][ch, 2 * q, pl.ds(sy, N), :], back, 1)
                b = pltpu.roll(pads[k][ch, 2 - q, pl.ds(sy, N), :], back, 1)
                wins[k, ch, p * N : (p + 1) * N] = jnp.where(lane_n < N - r, a, b)

    def incident(k):
        if k == 0:
            return tuple(jnp.concatenate([probe[c]] * B, axis=0) for c in range(2))
        return psi[k - 1, 0], psi[k - 1, 1]

    def exit_wave(k):
        ar, ai = incident(k)
        wr, wi = wins[k, 0], wins[k, 1]
        return ar * wr - ai * wi, ar * wi + ai * wr

    def forward(k):
        zr, zi = both_sides(*exit_wave(k), tab, 0, False)
        psi[k, 0] = zr
        psi[k, 1] = zi

    pack(0)
    pl.semaphore_wait(barrier, len(greet))
    send_rim(0, 0)
    middle_in(0)
    pack(1)
    send_rim(1, 0)
    middle_in(1)
    pack(2)
    middle_in(2)
    pack(3)
    middle_in(3)

    def clear(i, carry):
        zbuf[i] = jnp.zeros(zbuf.shape[1:], F32)
        return carry

    lax.fori_loop(0, zbuf.shape[0], clear, 0)
    for c in others:
        c.wait()

    merge(0, 0)
    send_rim(0, 1)
    send_rim(2, 0)
    relay_in(0)
    relay_in(1)
    merge(1, 0)
    send_rim(1, 1)
    send_rim(3, 0)
    relay_in(2)
    relay_in(3)
    merge(0, 1)
    merge(2, 0)
    send_rim(2, 1)
    windows(0)
    forward(0)
    merge(1, 1)
    merge(3, 0)
    send_rim(3, 1)
    windows(1)
    forward(1)
    merge(2, 1)
    windows(2)
    forward(2)
    merge(3, 1)
    windows(3)

    fr, fi = both_sides(*exit_wave(S - 1), tab, 1, False)
    level = jnp.concatenate([jnp.full((N, N), flags[p].astype(F32), F32) for p in range(B)], axis=0)
    excess = level * (fr * fr + fi * fi - inten[...])
    gr, gi = both_sides(excess * fr, excess * fi, tab, 1, True)

    def pack_cols(k, part):
        for ds, ts in ROWS[part]:
            rows = slice(M + ts.start, M + ts.stop)
            m = low_of(gpad[k, 0, 0, rows])
            cbuf[k, 0, ds] = jnp.where(m, gpad[k, 0, 0, rows], swap(gpad[k, 1, 0, rows]))
            cbuf[k, 1, ds] = jnp.where(m, swap(gpad[k, 0, 1, rows]), gpad[k, 1, 1, rows])
        rows = pl.ds(part * N, N)
        go(
            remote(cbuf.at[k, 0, rows], cgot.at[k, 1, rows], sent.at[2], cr.at[k, part], (me_r, left)),
            remote(cbuf.at[k, 1, rows], cgot.at[k, 0, rows], sent.at[2], cr.at[k, part], (me_r, right)),
        )

    def deposit(k, gr, gi):
        ar, ai = incident(k)
        for ch, g in enumerate((ar * gr + ai * gi, ar * gi - ai * gr)):
            for p in range(B):
                r = spots[p][2]
                g_p = pltpu.roll(g[p * N : (p + 1) * N], r, 1)
                zbuf[p * 2 + ch, 1, T : T + N] = jnp.where(lane_n >= r, g_p, 0.0)
                zbuf[p * 2 + ch, 2, T : T + N] = jnp.where(lane_n < r, g_p, 0.0)
        for ch in range(2):
            for j in range(3):
                acc = None
                for p in range(B):
                    sy, q, r = spots[p]
                    group = lax.rem(j + 1 - q + 3, 3)
                    piece = zbuf[p * 2 + ch, group, pl.ds(T - sy, T + N), :]
                    acc = piece if acc is None else acc + piece
                gpad[k, ch, (0, 2, 1)[j]] = acc
        send_rows(*out_args(k))
        send_middle(*out_args(k), S + k)
        pack_cols(k, 1)

    def fold_rows(k):
        drain(rbuf.at[k], rr.at[k])
        gpad[k, :, :, M : 2 * M] += rbuf[k, 0]
        gpad[k, :, :, T : T + M] += rbuf[k, 1]
        pack_cols(k, 0)

    for k in range(S - 1, -1, -1):
        deposit(k, gr, gi)
        wr, wi = wins[k, 0], wins[k, 1]
        gr, gi = wr * gr + wi * gi, wr * gi - wi * gr
        if k > 0:
            gr, gi = both_sides(gr, gi, tab, 0, True)
    for c, g in enumerate((gr, gi)):
        pgrad[c * N : (c + 1) * N] = (g[:N] + g[N : 2 * N]) + (g[2 * N : 3 * N] + g[3 * N :])

    D1 = 2 * N // G1
    D2 = D1 // YY

    def at(ref, i, depth):
        return ref.at[pl.ds(pl.multiple_of(i * depth, 8), depth)]

    def sum_of(ref):
        acc = ref[0]
        for i in range(1, ref.shape[0]):
            acc = acc + ref[i]
        return acc

    def arrive(stage, ref):
        drain(ref.at[pl.ds(0, ref.shape[0] - ref.shape[0] // COUNT[stage])], got.at[stage])

    COUNT = (G1, YY, 2 * ZH, YY, G1)
    go(*[
        remote(at(pgrad, j, D1), ar1.at[j1], sent.at[4], got.at[0], (zl * G1 + j, me_c))
        for j in group1
    ])
    ar1[j1] = pgrad[pl.ds(pl.multiple_of(j1 * D1, 8), D1), :]
    for k in range(S - 1, -1, -1):
        relay_out(k)
    arrive(0, ar1)
    part1[...] = sum_of(ar1)
    go(*[
        remote(at(part1, y, D2), ar2.at[yy], sent.at[5], got.at[1], (me_r, y * ZH + zh))
        for y in group2
    ])
    ar2[yy] = part1[pl.ds(pl.multiple_of(yy * D2, 8), D2), :]
    arrive(1, ar2)
    zz = zh * 2 + zl
    acc = sum_of(ar2)
    part2[...] = acc
    ar3[zz] = acc
    go(*[
        remote(part2, ar3.at[zz], sent.at[6], got.at[2], (a * G1 + j1, yy * ZH + b))
        for a, b in group3
    ])
    fold_rows(3)
    fold_rows(2)
    fold_rows(1)
    fold_rows(0)

    def finish(k):
        for part in range(2):
            drain(cgot.at[k, :, pl.ds(part * N, N)], cr.at[k, part])
            for ds, ts in ROWS[part]:
                lo, hi = cgot[k, 0, ds], cgot[k, 1, ds]
                rows = slice(M + ts.start, M + ts.stop)
                m = low_of(lo)
                for ch in range(2):
                    t0, t1, t2 = (swap(gpad[k, ch, j, rows]) for j in (0, 2, 1))
                    lo_c, hi_c = (lo, swap(hi)) if ch == 0 else (swap(lo), hi)
                    tile[k, ch, ts, :N] -= object_step * jnp.where(m, t0 + lo_c, t1)
                    tile[k, ch, ts, N:] -= object_step * jnp.where(m, t1, t2 + hi_c)
        c = pltpu.make_async_copy(tile.at[k], out_obj.at[k], out_sem.at[k])
        c.start()
        return c

    arrive(2, ar3)
    acc = sum_of(ar3)
    part3[...] = acc
    part4[pl.ds(pl.multiple_of(yy * D2, 8), D2), :] = acc
    go(*[
        remote(part3, at(part4, yy, D2), sent.at[7], got.at[3], (me_r, y * ZH + zh))
        for y in group2
    ])
    arrive(3, part4)
    go(*[
        remote(part4, at(total, j1, D1), sent.at[8], got.at[4], (zl * G1 + j, me_c))
        for j in group1
    ])
    total[pl.ds(pl.multiple_of(j1 * D1, 8), D1), :] = part4[...]
    stores = [finish(3), finish(2)]
    arrive(4, total)
    factor = 1.0 / math.sqrt(B * n_row * n_col)
    for c in range(2):
        out_probe[c] = probe[c] - factor * total[c * N : (c + 1) * N]
    stores += [finish(1), finish(0)]
    drain(sbuf, sent.at[0])

    @pl.when(jnp.logical_or(j1 == 2, j1 == G1 - 3))
    def _():
        drain(relay, relay_sent)

    drain(rbuf, sent.at[1])
    drain(cbuf, sent.at[2])
    drain(rbuf, sent.at[3])
    for stage, ref in enumerate((ar1, ar2, ar3, part4, total)):
        drain(ref.at[pl.ds(0, ref.shape[0] - ref.shape[0] // COUNT[stage])], sent.at[4 + stage])
    for c in stores:
        c.wait()


def body(n_row, n_col, object_slices, probe_wave, offsets, active_flags, intensity):
    vmem = pl.BlockSpec(memory_space=pltpu.VMEM)
    smem = pl.BlockSpec(memory_space=pltpu.SMEM)
    hbm = pl.BlockSpec(memory_space=pltpu.HBM)
    dma = pltpu.SemaphoreType.DMA

    def stay(x):
        return pltpu.with_memory_space_constraint(x, pltpu.HBM)

    scratch = (
        [
            pltpu.VMEM((S, 2, T, T), F32),
            pltpu.VMEM((2, N, N), F32),
            pltpu.VMEM((B * N, N), F32),
            pltpu.VMEM((2, 4, 2 * N, 2 * N), BF16),
        ]
        + [pltpu.VMEM((2, 3, T + N, N), F32)] * S
        + [
            pltpu.VMEM((S, 2, T, N), F32),
            pltpu.VMEM((S, 2, T, N), F32),
            pltpu.VMEM((S, 2, B * N, N), F32),
            pltpu.VMEM((S - 1, 2, B * N, N), F32),
            pltpu.VMEM((2 * B, 3, 2 * T + N, N), F32),
            pltpu.VMEM((S, 2, 3, T + N, N), F32),
            pltpu.VMEM((S, 2, 2, 3, M, N), F32),
            pltpu.VMEM((S, 2, T, N), F32),
            pltpu.VMEM((S, 2, T, N), F32),
            pltpu.VMEM((2 * N, N), F32),
            pltpu.VMEM((G1, 2 * N // G1, N), F32),
            pltpu.VMEM((YY, 8, N), F32),
            pltpu.VMEM((2 * ZH, 8, N), F32),
            pltpu.VMEM((2 * N // G1, N), F32),
            pltpu.VMEM((8, N), F32),
            pltpu.VMEM((8, N), F32),
            pltpu.VMEM((2 * N // G1, N), F32),
            pltpu.VMEM((2 * N, N), F32),
            pltpu.VMEM((2 * S, 2, M, N), F32),
        ]
        + [dma((S,)), dma((3,)), dma((S,)), dma((9,))]
        + [dma((S, 2)), dma((S,)), dma((S,)), dma((S, 2)), dma((5,)), dma((2 * S,)), dma]
    )
    return pl.pallas_call(
        functools.partial(kernel, n_row, n_col),
        out_shape=(
            jax.ShapeDtypeStruct((S, 2, T, T), F32),
            jax.ShapeDtypeStruct((2, N, N), F32),
        ),
        in_specs=[smem, smem, hbm, hbm, hbm, hbm],
        out_specs=(pl.BlockSpec(memory_space=pl.ANY), vmem),
        scratch_shapes=scratch,
        compiler_params=pltpu.CompilerParams(
            collective_id=0, has_side_effects=True, vmem_limit_bytes=VMEM_LIMIT
        ),
        name="step",
    )(
        stay(jnp.transpose(offsets.reshape(B, 2))),
        stay(active_flags.reshape(B)),
        stay(object_slices),
        stay(probe_wave),
        stay(intensity.reshape(B * N, N)),
        stay(jnp.asarray(tables())),
    )


def solution(mesh):
    in_specs = (
        P(None, None, "row", "col"),
        P(),
        P("row", "col", None, None),
        P("row", "col", None),
        P("row", "col", None, None, None),
    )
    out_specs = (P(None, None, "row", "col"), P())
    run = functools.partial(body, mesh.shape["row"], mesh.shape["col"])
    return jax.shard_map(run, mesh=mesh, in_specs=in_specs, out_specs=out_specs, check_vma=False)
```

```python
import functools
import math

import jax
import jax.numpy as jnp
import numpy as np
from jax import lax
from jax.experimental import pallas as pl
from jax.experimental.pallas import tpu as pltpu
from jax.sharding import PartitionSpec as P

fresnel_phase = 40.0
object_step = 0.25
N = 128
T = 256
M = 64
S = 4
B = 4
G1, YY, ZH = 8, 4, 4
RELAY_NEAR = True
VMEM_LIMIT = 52000000
F32 = jnp.float32
BF16 = jnp.bfloat16
MESH = pl.DeviceIdType.MESH


def block_pair(mat):
    re, im = mat.real, mat.imag
    right = np.block([[re, im], [-im, re]])
    left = np.block([[re, -im], [im, re]])
    out = []
    for block in (right, left):
        high = block.astype(np.float32).astype(BF16)
        low = (block - high.astype(np.float64)).astype(np.float32).astype(BF16)
        out += [high, low]
    return np.stack(out)


def tables():
    index = np.arange(N)
    dft = np.exp(-2j * np.pi * (index[:, None] * index[None, :] % N) / N) / math.sqrt(N)
    freq = ((index + N // 2) % N - N // 2) / N
    chirp = np.exp(-1j * np.pi * fresnel_phase * freq**2)
    hop = np.conj(dft) @ (chirp[:, None] * dft)
    return np.stack([block_pair(hop), block_pair(dft)])


def split(x):
    high = x.astype(BF16)
    return high, (x - high.astype(F32)).astype(BF16)


def dot(a, b):
    return jnp.dot(a, b, preferred_element_type=F32)


def both_sides(xr, xi, tab, which, conj):
    r, l = (2, 0) if conj else (0, 2)
    xh, xl = split(jnp.concatenate([xr, xi], axis=1))
    wh, wl = tab[which, r], tab[which, r + 1]
    y = dot(xh, wh) + (dot(xl, wh) + dot(xh, wl))
    cols = []
    for p in range(B):
        part = y[p * N : (p + 1) * N]
        cols.append(jnp.concatenate([part[:, :N], part[:, N:]], axis=0))
    yh, yl = split(jnp.concatenate(cols, axis=1))
    vh, vl = tab[which, l], tab[which, l + 1]
    z = dot(vh, yh) + (dot(vh, yl) + dot(vl, yh))
    zr = jnp.concatenate([z[:N, p * N : (p + 1) * N] for p in range(B)], axis=0)
    zi = jnp.concatenate([z[N:, p * N : (p + 1) * N] for p in range(B)], axis=0)
    return zr, zi


def kernel(
    n_row, n_col,
    offs_hbm, flags_hbm, obj_hbm, probe_hbm, inten_hbm, tab_hbm,
    out_obj, out_probe,
    tile, probe, inten, tab, pad0, pad1, pad2, pad3, halo, sbuf, wins, psi, zbuf, gpad, rbuf, cbuf, cgot,
    pgrad, ar1, ar2, ar3, part1, part2, part3, part4, total, relay, offs, flags,
    obj_sem, in_sem, out_sem, sent, hr, pr, rr, cr, got, relay_got, relay_sent,
):
    pads = (pad0, pad1, pad2, pad3)
    me_r = lax.axis_index("row")
    me_c = lax.axis_index("col")
    up, down = lax.rem(me_r + n_row - 1, n_row), lax.rem(me_r + 1, n_row)
    left, right = lax.rem(me_c + n_col - 1, n_col), lax.rem(me_c + 1, n_col)
    zl, j1 = lax.div(me_r, G1), lax.rem(me_r, G1)
    yy, zh = lax.div(me_c, ZH), lax.rem(me_c, ZH)
    group1 = [lax.rem(j1 + d, G1) for d in range(1, G1)]
    group2 = [lax.rem(yy + d, YY) for d in range(1, YY)]
    group3 = [(lax.rem(zl + a, 2), lax.rem(zh + b, ZH)) for a in range(2) for b in range(ZH) if a or b]
    low = lax.broadcasted_iota(jnp.int32, (T, N), 1) < M
    zo = 1 - zl
    z_relay, z_final = (zl, zo) if RELAY_NEAR else (zo, zl)
    relay_up, relay_down = z_relay * G1 + 2, z_relay * G1 + G1 - 3
    final_up, final_down = z_final * G1 + G1 - 1, z_final * G1

    def low_of(x):
        return low[: x.shape[0]]

    def swap(x):
        return pltpu.roll(x, M, 1)

    def remote(src, dst, ssem, rsem, dev):
        return pltpu.make_async_remote_copy(
            src_ref=src, dst_ref=dst, send_sem=ssem, recv_sem=rsem, device_id=dev, device_id_type=MESH
        )

    loads = [pltpu.make_async_copy(obj_hbm.at[k], tile.at[k], obj_sem.at[k]) for k in range(S)]
    for c in loads:
        c.start()
    others = [
        pltpu.make_async_copy(a, b, in_sem.at[i])
        for i, (a, b) in enumerate(
            ((offs_hbm, offs), (flags_hbm, flags), (probe_hbm, probe), (tab_hbm, tab), (inten_hbm, inten))
        )
    ]
    for c in others:
        c.start()
    barrier = pltpu.get_barrier_semaphore()
    greet = [(up, me_c), (down, me_c), (me_r, left), (me_r, right)]
    greet += [(zl * G1 + j, me_c) for j in group1]
    greet += [(me_r, y * ZH + zh) for y in group2]
    greet += [(a * G1 + j1, yy * ZH + b) for a, b in group3]
    reach = 3 if RELAY_NEAR else 2
    greet += [(zo * G1 + lax.rem(j1 + d, G1), me_c) for d in (reach, G1 - reach)]
    for dev in greet:
        pl.semaphore_signal(barrier, inc=1, device_id=dev, device_id_type=MESH)

    def go(*copies):
        for c in copies:
            c.start()

    def drain(ref, sem):
        pltpu.make_async_copy(ref, ref, sem).wait()

    PARTS = (slice(0, N), slice(N, T))
    ROWS = (((slice(0, M), slice(0, M)), (slice(M, N), slice(T - M, T))), ((slice(N, T), slice(M, T - M)),))

    def pack(k):
        loads[k].wait()
        for ds, ts in ROWS[0] + ROWS[1]:
            r0, r1 = tile[k, 0, ts, :N], tile[k, 0, ts, N:]
            i0, i1 = tile[k, 1, ts, :N], tile[k, 1, ts, N:]
            m = low_of(r0)
            sbuf[k, 0, ds] = jnp.where(m, r0, swap(i0))
            sbuf[k, 1, ds] = jnp.where(m, swap(r1), i1)
            rows = slice(M + ts.start, M + ts.stop)
            pads[k][0, 2, rows] = jnp.where(m, swap(r0), swap(r1))
            pads[k][1, 2, rows] = jnp.where(m, swap(i0), swap(i1))

    def send_rim(k, part):
        rows = pl.ds(part * N, N)
        go(
            remote(sbuf.at[k, 0, rows], halo.at[k, 1, rows], sent.at[0], hr.at[k, part], (me_r, left)),
            remote(sbuf.at[k, 1, rows], halo.at[k, 0, rows], sent.at[0], hr.at[k, part], (me_r, right)),
        )

    def send_rows(src, top, bottom, ssem, rsem):
        side = pl.ds(0, 2)
        go(
            remote(src.at[:, side, top[0]], top[1].at[:, side], ssem, rsem, (up, me_c)),
            remote(src.at[:, side, bottom[0]], bottom[1].at[:, side], ssem, rsem, (down, me_c)),
        )

    def send_middle(src, top, bottom, ssem, rsem, slot):
        for (rows, dst), edge, dev, hop in (
            (top, j1 == 0, up, relay_up), (bottom, j1 == G1 - 1, down, relay_down)
        ):
            @pl.when(edge)
            def _():
                remote(src.at[:, 2, rows], relay.at[slot], ssem, relay_got.at[slot], (hop, me_c)).start()

            @pl.when(jnp.logical_not(edge))
            def _():
                remote(src.at[:, 2, rows], dst.at[:, 2], ssem, rsem, (dev, me_c)).start()

    def pass_on(top, bottom, rsem, slot):
        for dst, here, dev in ((top, j1 == 2, final_up), (bottom, j1 == G1 - 3, final_down)):
            @pl.when(here)
            def _():
                drain(relay.at[slot], relay_got.at[slot])
                remote(relay.at[slot], dst.at[:, 2], relay_sent, rsem, (dev, me_c)).start()

    def in_top(k):
        return pads[k].at[:, :, pl.ds(M + T, M)]

    def in_bottom(k):
        return pads[k].at[:, :, pl.ds(0, M)]

    def in_args(k):
        return pads[k], (pl.ds(M, M), in_top(k)), (pl.ds(T, M), in_bottom(k)), sent.at[1], pr.at[k]

    def middle_in(k):
        send_middle(*in_args(k), k)

    def relay_in(k):
        pass_on(in_top(k), in_bottom(k), pr.at[k], k)

    def out_args(k):
        return (
            gpad.at[k], (pl.ds(0, M), rbuf.at[k, 1]), (pl.ds(M + T, M), rbuf.at[k, 0]), sent.at[3], rr.at[k]
        )

    def relay_out(k):
        pass_on(rbuf.at[k, 1], rbuf.at[k, 0], rr.at[k], S + k)

    def merge(k, part):
        drain(halo.at[k, :, pl.ds(part * N, N)], hr.at[k, part])
        for ds, ts in ROWS[part]:
            lo, hi = halo[k, 0, ds], halo[k, 1, ds]
            m = low_of(lo)
            rows = slice(M + ts.start, M + ts.stop)
            pads[k][0, 0, rows] = jnp.where(m, lo, swap(tile[k, 0, ts, :N]))
            pads[k][1, 0, rows] = jnp.where(m, swap(lo), swap(tile[k, 1, ts, :N]))
            pads[k][0, 1, rows] = jnp.where(m, swap(tile[k, 0, ts, N:]), swap(hi))
            pads[k][1, 1, rows] = jnp.where(m, swap(tile[k, 1, ts, N:]), hi)
        if part == 0:
            send_rows(*in_args(k))

    lane_n = lax.broadcasted_iota(jnp.int32, (N, N), 1)
    spots = []

    def windows(k):
        drain(rbuf.at[k], pr.at[k])
        for p in range(B):
            sy, q, r = spots[p]
            back = lax.bitwise_and(N - r, N - 1)
            for ch in range(2):
                a = pltpu.roll(pads[k][ch, 2 * q, pl.ds(sy, N), :], back, 1)
                b = pltpu.roll(pads[k][ch, 2 - q, pl.ds(sy, N), :], back, 1)
                wins[k, ch, p * N : (p + 1) * N] = jnp.where(lane_n < N - r, a, b)

    def incident(k):
        if k == 0:
            return tuple(jnp.concatenate([probe[c]] * B, axis=0) for c in range(2))
        return psi[k - 1, 0], psi[k - 1, 1]

    def exit_wave(k):
        ar, ai = incident(k)
        wr, wi = wins[k, 0], wins[k, 1]
        return ar * wr - ai * wi, ar * wi + ai * wr

    def forward(k):
        zr, zi = both_sides(*exit_wave(k), tab, 0, False)
        psi[k, 0] = zr
        psi[k, 1] = zi

    pack(0)
    pl.semaphore_wait(barrier, len(greet))
    send_rim(0, 0)
    middle_in(0)
    pack(1)
    send_rim(1, 0)
    middle_in(1)
    pack(2)
    middle_in(2)
    pack(3)
    middle_in(3)

    def clear(i, carry):
        zbuf[i] = jnp.zeros(zbuf.shape[1:], F32)
        return carry

    lax.fori_loop(0, zbuf.shape[0], clear, 0)
    for c in others:
        c.wait()
    for p in range(B):
        sy, sx = offs[0, p], offs[1, p]
        spots.append((sy, lax.shift_right_logical(sx, 7), lax.bitwise_and(sx, N - 1)))

    merge(0, 0)
    send_rim(0, 1)
    send_rim(2, 0)
    relay_in(0)
    relay_in(1)
    merge(1, 0)
    send_rim(1, 1)
    send_rim(3, 0)
    relay_in(2)
    relay_in(3)
    merge(0, 1)
    merge(2, 0)
    send_rim(2, 1)
    windows(0)
    forward(0)
    merge(1, 1)
    merge(3, 0)
    send_rim(3, 1)
    windows(1)
    forward(1)
    merge(2, 1)
    windows(2)
    forward(2)
    merge(3, 1)
    windows(3)

    fr, fi = both_sides(*exit_wave(S - 1), tab, 1, False)
    level = jnp.concatenate([jnp.full((N, N), flags[p].astype(F32), F32) for p in range(B)], axis=0)
    excess = level * (fr * fr + fi * fi - inten[...])
    gr, gi = both_sides(excess * fr, excess * fi, tab, 1, True)

    def pack_cols(k, part):
        for ds, ts in ROWS[part]:
            rows = slice(M + ts.start, M + ts.stop)
            m = low_of(gpad[k, 0, 0, rows])
            cbuf[k, 0, ds] = jnp.where(m, gpad[k, 0, 0, rows], swap(gpad[k, 1, 0, rows]))
            cbuf[k, 1, ds] = jnp.where(m, swap(gpad[k, 0, 1, rows]), gpad[k, 1, 1, rows])
        rows = pl.ds(part * N, N)
        go(
            remote(cbuf.at[k, 0, rows], cgot.at[k, 1, rows], sent.at[2], cr.at[k, part], (me_r, left)),
            remote(cbuf.at[k, 1, rows], cgot.at[k, 0, rows], sent.at[2], cr.at[k, part], (me_r, right)),
        )

    def deposit(k, gr, gi):
        ar, ai = incident(k)
        for ch, g in enumerate((ar * gr + ai * gi, ar * gi - ai * gr)):
            for p in range(B):
                r = spots[p][2]
                g_p = pltpu.roll(g[p * N : (p + 1) * N], r, 1)
                zbuf[p * 2 + ch, 1, T : T + N] = jnp.where(lane_n >= r, g_p, 0.0)
                zbuf[p * 2 + ch, 2, T : T + N] = jnp.where(lane_n < r, g_p, 0.0)
        for ch in range(2):
            for j in range(3):
                acc = None
                for p in range(B):
                    sy, q, r = spots[p]
                    group = lax.rem(j + 1 - q + 3, 3)
                    piece = zbuf[p * 2 + ch, group, pl.ds(T - sy, T + N), :]
                    acc = piece if acc is None else acc + piece
                gpad[k, ch, (0, 2, 1)[j]] = acc
        send_rows(*out_args(k))
        send_middle(*out_args(k), S + k)
        pack_cols(k, 1)

    def fold_rows(k):
        drain(rbuf.at[k], rr.at[k])
        gpad[k, :, :, M : 2 * M] += rbuf[k, 0]
        gpad[k, :, :, T : T + M] += rbuf[k, 1]
        pack_cols(k, 0)

    for k in range(S - 1, -1, -1):
        deposit(k, gr, gi)
        wr, wi = wins[k, 0], wins[k, 1]
        gr, gi = wr * gr + wi * gi, wr * gi - wi * gr
        if k > 0:
            gr, gi = both_sides(gr, gi, tab, 0, True)
    for c, g in enumerate((gr, gi)):
        pgrad[c * N : (c + 1) * N] = (g[:N] + g[N : 2 * N]) + (g[2 * N : 3 * N] + g[3 * N :])

    D1 = 2 * N // G1
    D2 = D1 // YY

    def at(ref, i, depth):
        return ref.at[pl.ds(pl.multiple_of(i * depth, 8), depth)]

    def sum_of(ref):
        acc = ref[0]
        for i in range(1, ref.shape[0]):
            acc = acc + ref[i]
        return acc

    def arrive(stage, ref):
        drain(ref.at[pl.ds(0, ref.shape[0] - ref.shape[0] // COUNT[stage])], got.at[stage])

    COUNT = (G1, YY, 2 * ZH, YY, G1)
    go(*[
        remote(at(pgrad, j, D1), ar1.at[j1], sent.at[4], got.at[0], (zl * G1 + j, me_c))
        for j in group1
    ])
    ar1[j1] = pgrad[pl.ds(pl.multiple_of(j1 * D1, 8), D1), :]
    for k in range(S - 1, -1, -1):
        relay_out(k)
    arrive(0, ar1)
    part1[...] = sum_of(ar1)
    go(*[
        remote(at(part1, y, D2), ar2.at[yy], sent.at[5], got.at[1], (me_r, y * ZH + zh))
        for y in group2
    ])
    ar2[yy] = part1[pl.ds(pl.multiple_of(yy * D2, 8), D2), :]
    arrive(1, ar2)
    zz = zh * 2 + zl
    acc = sum_of(ar2)
    part2[...] = acc
    ar3[zz] = acc
    go(*[
        remote(part2, ar3.at[zz], sent.at[6], got.at[2], (a * G1 + j1, yy * ZH + b))
        for a, b in group3
    ])
    fold_rows(3)
    fold_rows(2)
    fold_rows(1)
    fold_rows(0)

    def finish(k):
        for part in range(2):
            drain(cgot.at[k, :, pl.ds(part * N, N)], cr.at[k, part])
            for ds, ts in ROWS[part]:
                lo, hi = cgot[k, 0, ds], cgot[k, 1, ds]
                rows = slice(M + ts.start, M + ts.stop)
                m = low_of(lo)
                for ch in range(2):
                    t0, t1, t2 = (swap(gpad[k, ch, j, rows]) for j in (0, 2, 1))
                    lo_c, hi_c = (lo, swap(hi)) if ch == 0 else (swap(lo), hi)
                    tile[k, ch, ts, :N] -= object_step * jnp.where(m, t0 + lo_c, t1)
                    tile[k, ch, ts, N:] -= object_step * jnp.where(m, t1, t2 + hi_c)
        c = pltpu.make_async_copy(tile.at[k], out_obj.at[k], out_sem.at[k])
        c.start()
        return c

    arrive(2, ar3)
    acc = sum_of(ar3)
    part3[...] = acc
    part4[pl.ds(pl.multiple_of(yy * D2, 8), D2), :] = acc
    go(*[
        remote(part3, at(part4, yy, D2), sent.at[7], got.at[3], (me_r, y * ZH + zh))
        for y in group2
    ])
    arrive(3, part4)
    go(*[
        remote(part4, at(total, j1, D1), sent.at[8], got.at[4], (zl * G1 + j, me_c))
        for j in group1
    ])
    total[pl.ds(pl.multiple_of(j1 * D1, 8), D1), :] = part4[...]
    stores = [finish(3), finish(2)]
    arrive(4, total)
    factor = 1.0 / math.sqrt(B * n_row * n_col)
    for c in range(2):
        out_probe[c] = probe[c] - factor * total[c * N : (c + 1) * N]
    stores += [finish(1), finish(0)]
    drain(sbuf, sent.at[0])

    @pl.when(jnp.logical_or(j1 == 2, j1 == G1 - 3))
    def _():
        drain(relay, relay_sent)

    drain(rbuf, sent.at[1])
    drain(cbuf, sent.at[2])
    drain(rbuf, sent.at[3])
    for stage, ref in enumerate((ar1, ar2, ar3, part4, total)):
        drain(ref.at[pl.ds(0, ref.shape[0] - ref.shape[0] // COUNT[stage])], sent.at[4 + stage])
    for c in stores:
        c.wait()


def body(n_row, n_col, object_slices, probe_wave, offsets, active_flags, intensity):
    vmem = pl.BlockSpec(memory_space=pltpu.VMEM)
    smem = pl.BlockSpec(memory_space=pltpu.SMEM)
    hbm = pl.BlockSpec(memory_space=pltpu.HBM)
    dma = pltpu.SemaphoreType.DMA

    def stay(x):
        return pltpu.with_memory_space_constraint(x, pltpu.HBM)

    scratch = (
        [
            pltpu.VMEM((S, 2, T, T), F32),
            pltpu.VMEM((2, N, N), F32),
            pltpu.VMEM((B * N, N), F32),
            pltpu.VMEM((2, 4, 2 * N, 2 * N), BF16),
        ]
        + [pltpu.VMEM((2, 3, T + N, N), F32)] * S
        + [
            pltpu.VMEM((S, 2, T, N), F32),
            pltpu.VMEM((S, 2, T, N), F32),
            pltpu.VMEM((S, 2, B * N, N), F32),
            pltpu.VMEM((S - 1, 2, B * N, N), F32),
            pltpu.VMEM((2 * B, 3, 2 * T + N, N), F32),
            pltpu.VMEM((S, 2, 3, T + N, N), F32),
            pltpu.VMEM((S, 2, 2, 3, M, N), F32),
            pltpu.VMEM((S, 2, T, N), F32),
            pltpu.VMEM((S, 2, T, N), F32),
            pltpu.VMEM((2 * N, N), F32),
            pltpu.VMEM((G1, 2 * N // G1, N), F32),
            pltpu.VMEM((YY, 8, N), F32),
            pltpu.VMEM((2 * ZH, 8, N), F32),
            pltpu.VMEM((2 * N // G1, N), F32),
            pltpu.VMEM((8, N), F32),
            pltpu.VMEM((8, N), F32),
            pltpu.VMEM((2 * N // G1, N), F32),
            pltpu.VMEM((2 * N, N), F32),
            pltpu.VMEM((2 * S, 2, M, N), F32),
            pltpu.SMEM((2, B), jnp.int32),
            pltpu.SMEM((B,), jnp.int32),
        ]
        + [dma((S,)), dma((5,)), dma((S,)), dma((9,))]
        + [dma((S, 2)), dma((S,)), dma((S,)), dma((S, 2)), dma((5,)), dma((2 * S,)), dma]
    )
    return pl.pallas_call(
        functools.partial(kernel, n_row, n_col),
        out_shape=(
            jax.ShapeDtypeStruct((S, 2, T, T), F32),
            jax.ShapeDtypeStruct((2, N, N), F32),
        ),
        in_specs=[hbm, hbm, hbm, hbm, hbm, hbm],
        out_specs=(pl.BlockSpec(memory_space=pl.ANY), vmem),
        scratch_shapes=scratch,
        compiler_params=pltpu.CompilerParams(
            collective_id=0, has_side_effects=True, vmem_limit_bytes=VMEM_LIMIT
        ),
        name="step",
    )(
        stay(jnp.transpose(offsets.reshape(B, 2))),
        stay(active_flags.reshape(B)),
        stay(object_slices),
        stay(probe_wave),
        stay(intensity.reshape(B * N, N)),
        stay(jnp.asarray(tables())),
    )


def solution(mesh):
    in_specs = (
        P(None, None, "row", "col"),
        P(),
        P("row", "col", None, None),
        P("row", "col", None),
        P("row", "col", None, None, None),
    )
    out_specs = (P(None, None, "row", "col"), P())
    run = functools.partial(body, mesh.shape["row"], mesh.shape["col"])
    return jax.shard_map(run, mesh=mesh, in_specs=in_specs, out_specs=out_specs, check_vma=False)
```

```python
import functools
import math

import jax
import jax.numpy as jnp
import numpy as np
from jax import lax
from jax.experimental import pallas as pl
from jax.experimental.pallas import tpu as pltpu
from jax.sharding import PartitionSpec as P

fresnel_phase = 40.0
object_step = 0.25
N = 128
T = 256
M = 64
S = 4
B = 4
G1, YY, ZH = 8, 4, 4
RELAY_NEAR = True
VMEM_LIMIT = 52000000
F32 = jnp.float32
BF16 = jnp.bfloat16
MESH = pl.DeviceIdType.MESH


def block_pair(mat):
    re, im = mat.real, mat.imag
    right = np.block([[re, im], [-im, re]])
    left = np.block([[re, -im], [im, re]])
    out = []
    for block in (right, left):
        high = block.astype(np.float32).astype(BF16)
        low = (block - high.astype(np.float64)).astype(np.float32).astype(BF16)
        out += [high, low]
    return np.stack(out)


def tables():
    index = np.arange(N)
    dft = np.exp(-2j * np.pi * (index[:, None] * index[None, :] % N) / N) / math.sqrt(N)
    freq = ((index + N // 2) % N - N // 2) / N
    chirp = np.exp(-1j * np.pi * fresnel_phase * freq**2)
    hop = np.conj(dft) @ (chirp[:, None] * dft)
    return np.stack([block_pair(hop), block_pair(dft)])


def split(x):
    high = x.astype(BF16)
    return high, (x - high.astype(F32)).astype(BF16)


def dot(a, b):
    return jnp.dot(a, b, preferred_element_type=F32)


def both_sides(xr, xi, tab, which, conj):
    r, l = (2, 0) if conj else (0, 2)
    xh, xl = split(jnp.concatenate([xr, xi], axis=1))
    wh, wl = tab[which, r], tab[which, r + 1]
    y = dot(xh, wh) + (dot(xl, wh) + dot(xh, wl))
    cols = []
    for p in range(B):
        part = y[p * N : (p + 1) * N]
        cols.append(jnp.concatenate([part[:, :N], part[:, N:]], axis=0))
    yh, yl = split(jnp.concatenate(cols, axis=1))
    vh, vl = tab[which, l], tab[which, l + 1]
    z = dot(vh, yh) + (dot(vh, yl) + dot(vl, yh))
    zr = jnp.concatenate([z[:N, p * N : (p + 1) * N] for p in range(B)], axis=0)
    zi = jnp.concatenate([z[N:, p * N : (p + 1) * N] for p in range(B)], axis=0)
    return zr, zi


def kernel(
    n_row, n_col,
    offs_hbm, flags_hbm, obj_hbm, probe_hbm, inten_hbm, tab_hbm,
    out_obj, out_probe,
    tile, probe, inten, tab, pad0, pad1, pad2, pad3, halo, sbuf, wins, psi, zbuf, gpad, rbuf, cbuf, cgot,
    pgrad, ar1, ar2, ar3, part1, part2, part3, part4, total, relay, offs, flags,
    obj_sem, in_sem, out_sem, sent, hr, pr, rr, cr, got, relay_got, relay_sent,
):
    pads = (pad0, pad1, pad2, pad3)
    me_r = lax.axis_index("row")
    me_c = lax.axis_index("col")
    up, down = lax.rem(me_r + n_row - 1, n_row), lax.rem(me_r + 1, n_row)
    left, right = lax.rem(me_c + n_col - 1, n_col), lax.rem(me_c + 1, n_col)
    zl, j1 = lax.div(me_r, G1), lax.rem(me_r, G1)
    yy, zh = lax.div(me_c, ZH), lax.rem(me_c, ZH)
    group1 = [lax.rem(j1 + d, G1) for d in range(1, G1)]
    group2 = [lax.rem(yy + d, YY) for d in range(1, YY)]
    group3 = [(lax.rem(zl + a, 2), lax.rem(zh + b, ZH)) for a in range(2) for b in range(ZH) if a or b]
    low = lax.broadcasted_iota(jnp.int32, (T, N), 1) < M
    zo = 1 - zl
    z_relay, z_final = (zl, zo) if RELAY_NEAR else (zo, zl)
    relay_up, relay_down = z_relay * G1 + 2, z_relay * G1 + G1 - 3
    final_up, final_down = z_final * G1 + G1 - 1, z_final * G1

    def low_of(x):
        return low[: x.shape[0]]

    def swap(x):
        return pltpu.roll(x, M, 1)

    def remote(src, dst, ssem, rsem, dev):
        return pltpu.make_async_remote_copy(
            src_ref=src, dst_ref=dst, send_sem=ssem, recv_sem=rsem, device_id=dev, device_id_type=MESH
        )

    loads = [pltpu.make_async_copy(obj_hbm.at[k], tile.at[k], obj_sem.at[k]) for k in range(S)]
    for c in loads:
        c.start()
    others = [
        pltpu.make_async_copy(a, b, in_sem.at[i])
        for i, (a, b) in enumerate(
            ((offs_hbm, offs), (flags_hbm, flags), (probe_hbm, probe), (tab_hbm, tab), (inten_hbm, inten))
        )
    ]
    for c in others:
        c.start()
    barrier = pltpu.get_barrier_semaphore()
    greet = [(up, me_c), (down, me_c), (me_r, left), (me_r, right)]
    greet += [(zl * G1 + j, me_c) for j in group1]
    greet += [(me_r, y * ZH + zh) for y in group2]
    greet += [(a * G1 + j1, yy * ZH + b) for a, b in group3]
    reach = 3 if RELAY_NEAR else 2
    greet += [(zo * G1 + lax.rem(j1 + d, G1), me_c) for d in (reach, G1 - reach)]
    for dev in greet:
        pl.semaphore_signal(barrier, inc=1, device_id=dev, device_id_type=MESH)

    def go(*copies):
        for c in copies:
            c.start()

    def drain(ref, sem):
        pltpu.make_async_copy(ref, ref, sem).wait()

    PARTS = (slice(0, N), slice(N, T))
    ROWS = (((slice(0, M), slice(0, M)), (slice(M, N), slice(T - M, T))), ((slice(N, T), slice(M, T - M)),))

    def pack(k):
        loads[k].wait()
        for ds, ts in ROWS[0] + ROWS[1]:
            r0, r1 = tile[k, 0, ts, :N], tile[k, 0, ts, N:]
            i0, i1 = tile[k, 1, ts, :N], tile[k, 1, ts, N:]
            m = low_of(r0)
            sbuf[k, 0, ds] = jnp.where(m, r0, swap(i0))
            sbuf[k, 1, ds] = jnp.where(m, swap(r1), i1)
            rows = slice(M + ts.start, M + ts.stop)
            pads[k][0, 2, rows] = jnp.where(m, swap(r0), swap(r1))
            pads[k][1, 2, rows] = jnp.where(m, swap(i0), swap(i1))

    def send_rim(k, part):
        rows = pl.ds(part * N, N)
        go(
            remote(sbuf.at[k, 0, rows], halo.at[k, 1, rows], sent.at[0], hr.at[k, part], (me_r, left)),
            remote(sbuf.at[k, 1, rows], halo.at[k, 0, rows], sent.at[0], hr.at[k, part], (me_r, right)),
        )

    def send_rows(src, top, bottom, ssem, rsem):
        side = pl.ds(0, 2)
        go(
            remote(src.at[:, side, top[0]], top[1].at[:, side], ssem, rsem, (up, me_c)),
            remote(src.at[:, side, bottom[0]], bottom[1].at[:, side], ssem, rsem, (down, me_c)),
        )

    def send_middle(src, top, bottom, ssem, rsem, slot):
        for (rows, dst), edge, dev, hop in (
            (top, j1 == 0, up, relay_up), (bottom, j1 == G1 - 1, down, relay_down)
        ):
            @pl.when(edge)
            def _():
                remote(src.at[:, 2, rows], relay.at[slot], ssem, relay_got.at[slot], (hop, me_c)).start()

            @pl.when(jnp.logical_not(edge))
            def _():
                remote(src.at[:, 2, rows], dst.at[:, 2], ssem, rsem, (dev, me_c)).start()

    def pass_on(top, bottom, rsem, slot):
        for dst, here, dev in ((top, j1 == 2, final_up), (bottom, j1 == G1 - 3, final_down)):
            @pl.when(here)
            def _():
                drain(relay.at[slot], relay_got.at[slot])
                remote(relay.at[slot], dst.at[:, 2], relay_sent, rsem, (dev, me_c)).start()

    def in_top(k):
        return pads[k].at[:, :, pl.ds(M + T, M)]

    def in_bottom(k):
        return pads[k].at[:, :, pl.ds(0, M)]

    def in_args(k):
        return pads[k], (pl.ds(M, M), in_top(k)), (pl.ds(T, M), in_bottom(k)), sent.at[1], pr.at[k]

    def middle_in(k):
        send_middle(*in_args(k), k)

    def relay_in(k):
        pass_on(in_top(k), in_bottom(k), pr.at[k], k)

    def out_args(k):
        return (
            gpad.at[k], (pl.ds(0, M), rbuf.at[k, 1]), (pl.ds(M + T, M), rbuf.at[k, 0]), sent.at[3], rr.at[k]
        )

    def relay_out(k):
        pass_on(rbuf.at[k, 1], rbuf.at[k, 0], rr.at[k], S + k)

    def merge(k, part):
        drain(halo.at[k, :, pl.ds(part * N, N)], hr.at[k, part])
        for ds, ts in ROWS[part]:
            lo, hi = halo[k, 0, ds], halo[k, 1, ds]
            m = low_of(lo)
            rows = slice(M + ts.start, M + ts.stop)
            pads[k][0, 0, rows] = jnp.where(m, lo, swap(tile[k, 0, ts, :N]))
            pads[k][1, 0, rows] = jnp.where(m, swap(lo), swap(tile[k, 1, ts, :N]))
            pads[k][0, 1, rows] = jnp.where(m, swap(tile[k, 0, ts, N:]), swap(hi))
            pads[k][1, 1, rows] = jnp.where(m, swap(tile[k, 1, ts, N:]), hi)
        if part == 0:
            send_rows(*in_args(k))

    lane_n = lax.broadcasted_iota(jnp.int32, (N, N), 1)
    spots = []

    def windows(k):
        drain(rbuf.at[k], pr.at[k])
        for p in range(B):
            sy, q, r = spots[p]
            back = lax.bitwise_and(N - r, N - 1)
            for ch in range(2):
                a = pltpu.roll(pads[k][ch, 2 * q, pl.ds(sy, N), :], back, 1)
                b = pltpu.roll(pads[k][ch, 2 - q, pl.ds(sy, N), :], back, 1)
                wins[k, ch, p * N : (p + 1) * N] = jnp.where(lane_n < N - r, a, b)

    def incident(k):
        if k == 0:
            return tuple(jnp.concatenate([probe[c]] * B, axis=0) for c in range(2))
        return psi[k - 1, 0], psi[k - 1, 1]

    def exit_wave(k):
        ar, ai = incident(k)
        wr, wi = wins[k, 0], wins[k, 1]
        return ar * wr - ai * wi, ar * wi + ai * wr

    def forward(k):
        zr, zi = both_sides(*exit_wave(k), tab, 0, False)
        psi[k, 0] = zr
        psi[k, 1] = zi

    pack(0)
    pl.semaphore_wait(barrier, len(greet))
    send_rim(0, 0)
    middle_in(0)
    pack(1)
    send_rim(1, 0)
    middle_in(1)
    pack(2)
    middle_in(2)
    pack(3)
    middle_in(3)

    def clear(i, carry):
        zbuf[i] = jnp.zeros(zbuf.shape[1:], F32)
        return carry

    lax.fori_loop(0, zbuf.shape[0], clear, 0)
    for c in others:
        c.wait()
    for p in range(B):
        sy, sx = offs[0, p], offs[1, p]
        spots.append((sy, lax.shift_right_logical(sx, 7), lax.bitwise_and(sx, N - 1)))

    merge(0, 0)
    send_rim(0, 1)
    send_rim(2, 0)
    relay_in(0)
    relay_in(1)
    merge(1, 0)
    send_rim(1, 1)
    send_rim(3, 0)
    relay_in(2)
    relay_in(3)
    merge(0, 1)
    merge(2, 0)
    send_rim(2, 1)
    windows(0)
    forward(0)
    merge(1, 1)
    merge(3, 0)
    send_rim(3, 1)
    windows(1)
    forward(1)
    merge(2, 1)
    windows(2)
    forward(2)
    merge(3, 1)
    windows(3)

    fr, fi = both_sides(*exit_wave(S - 1), tab, 1, False)
    level = jnp.concatenate([jnp.full((N, N), flags[p].astype(F32), F32) for p in range(B)], axis=0)
    excess = level * (fr * fr + fi * fi - inten[...])
    gr, gi = both_sides(excess * fr, excess * fi, tab, 1, True)

    def pack_cols(k, part):
        for ds, ts in ROWS[part]:
            rows = slice(M + ts.start, M + ts.stop)
            m = low_of(gpad[k, 0, 0, rows])
            cbuf[k, 0, ds] = jnp.where(m, gpad[k, 0, 0, rows], swap(gpad[k, 1, 0, rows]))
            cbuf[k, 1, ds] = jnp.where(m, swap(gpad[k, 0, 1, rows]), gpad[k, 1, 1, rows])
        rows = pl.ds(part * N, N)
        go(
            remote(cbuf.at[k, 0, rows], cgot.at[k, 1, rows], sent.at[2], cr.at[k, part], (me_r, left)),
            remote(cbuf.at[k, 1, rows], cgot.at[k, 0, rows], sent.at[2], cr.at[k, part], (me_r, right)),
        )

    def deposit(k, gr, gi):
        ar, ai = incident(k)
        for ch, g in enumerate((ar * gr + ai * gi, ar * gi - ai * gr)):
            for p in range(B):
                r = spots[p][2]
                g_p = pltpu.roll(g[p * N : (p + 1) * N], r, 1)
                zbuf[p * 2 + ch, 1, T : T + N] = jnp.where(lane_n >= r, g_p, 0.0)
                zbuf[p * 2 + ch, 2, T : T + N] = jnp.where(lane_n < r, g_p, 0.0)
        for ch in range(2):
            for j in range(3):
                acc = None
                for p in range(B):
                    sy, q, r = spots[p]
                    group = lax.rem(j + 1 - q + 3, 3)
                    piece = zbuf[p * 2 + ch, group, pl.ds(T - sy, T + N), :]
                    acc = piece if acc is None else acc + piece
                gpad[k, ch, (0, 2, 1)[j]] = acc
        send_rows(*out_args(k))
        send_middle(*out_args(k), S + k)
        pack_cols(k, 1)

    def fold_rows(k):
        drain(rbuf.at[k], rr.at[k])
        gpad[k, :, :, M : 2 * M] += rbuf[k, 0]
        gpad[k, :, :, T : T + M] += rbuf[k, 1]
        pack_cols(k, 0)

    for k in range(S - 1, -1, -1):
        deposit(k, gr, gi)
        wr, wi = wins[k, 0], wins[k, 1]
        gr, gi = wr * gr + wi * gi, wr * gi - wi * gr
        if k > 0:
            gr, gi = both_sides(gr, gi, tab, 0, True)
    for c, g in enumerate((gr, gi)):
        pgrad[c * N : (c + 1) * N] = (g[:N] + g[N : 2 * N]) + (g[2 * N : 3 * N] + g[3 * N :])

    D1 = 2 * N // G1
    D2 = D1 // YY

    def at(ref, i, depth):
        return ref.at[pl.ds(pl.multiple_of(i * depth, 8), depth)]

    def sum_of(ref):
        acc = ref[0]
        for i in range(1, ref.shape[0]):
            acc = acc + ref[i]
        return acc

    def arrive(stage, ref):
        drain(ref.at[pl.ds(0, ref.shape[0] - ref.shape[0] // COUNT[stage])], got.at[stage])

    COUNT = (G1, YY, 2 * ZH, YY, G1)
    go(*[
        remote(at(pgrad, j, D1), ar1.at[j1], sent.at[4], got.at[0], (zl * G1 + j, me_c))
        for j in group1
    ])
    ar1[j1] = pgrad[pl.ds(pl.multiple_of(j1 * D1, 8), D1), :]
    for k in range(S - 1, -1, -1):
        relay_out(k)
    arrive(0, ar1)
    part1[...] = sum_of(ar1)
    go(*[
        remote(at(part1, y, D2), ar2.at[yy], sent.at[5], got.at[1], (me_r, y * ZH + zh))
        for y in group2
    ])
    ar2[yy] = part1[pl.ds(pl.multiple_of(yy * D2, 8), D2), :]
    arrive(1, ar2)
    zz = zh * 2 + zl
    acc = sum_of(ar2)
    part2[...] = acc
    ar3[zz] = acc
    go(*[
        remote(part2, ar3.at[zz], sent.at[6], got.at[2], (a * G1 + j1, yy * ZH + b))
        for a, b in group3
    ])
    fold_rows(3)
    fold_rows(2)
    fold_rows(1)
    fold_rows(0)

    def finish(k):
        for part in (1, 0):
            drain(cgot.at[k, :, pl.ds(part * N, N)], cr.at[k, part])
            for ds, ts in ROWS[part]:
                lo, hi = cgot[k, 0, ds], cgot[k, 1, ds]
                rows = slice(M + ts.start, M + ts.stop)
                m = low_of(lo)
                for ch in range(2):
                    t0, t1, t2 = (swap(gpad[k, ch, j, rows]) for j in (0, 2, 1))
                    lo_c, hi_c = (lo, swap(hi)) if ch == 0 else (swap(lo), hi)
                    tile[k, ch, ts, :N] -= object_step * jnp.where(m, t0 + lo_c, t1)
                    tile[k, ch, ts, N:] -= object_step * jnp.where(m, t1, t2 + hi_c)
        c = pltpu.make_async_copy(tile.at[k], out_obj.at[k], out_sem.at[k])
        c.start()
        return c

    arrive(2, ar3)
    acc = sum_of(ar3)
    part3[...] = acc
    part4[pl.ds(pl.multiple_of(yy * D2, 8), D2), :] = acc
    go(*[
        remote(part3, at(part4, yy, D2), sent.at[7], got.at[3], (me_r, y * ZH + zh))
        for y in group2
    ])
    arrive(3, part4)
    go(*[
        remote(part4, at(total, j1, D1), sent.at[8], got.at[4], (zl * G1 + j, me_c))
        for j in group1
    ])
    total[pl.ds(pl.multiple_of(j1 * D1, 8), D1), :] = part4[...]
    stores = [finish(3), finish(2)]
    arrive(4, total)
    factor = 1.0 / math.sqrt(B * n_row * n_col)
    for c in range(2):
        out_probe[c] = probe[c] - factor * total[c * N : (c + 1) * N]
    stores += [finish(1), finish(0)]
    drain(sbuf, sent.at[0])

    @pl.when(jnp.logical_or(j1 == 2, j1 == G1 - 3))
    def _():
        drain(relay, relay_sent)

    drain(rbuf, sent.at[1])
    drain(cbuf, sent.at[2])
    drain(rbuf, sent.at[3])
    for stage, ref in enumerate((ar1, ar2, ar3, part4, total)):
        drain(ref.at[pl.ds(0, ref.shape[0] - ref.shape[0] // COUNT[stage])], sent.at[4 + stage])
    for c in stores:
        c.wait()


def body(n_row, n_col, object_slices, probe_wave, offsets, active_flags, intensity):
    vmem = pl.BlockSpec(memory_space=pltpu.VMEM)
    smem = pl.BlockSpec(memory_space=pltpu.SMEM)
    hbm = pl.BlockSpec(memory_space=pltpu.HBM)
    dma = pltpu.SemaphoreType.DMA

    def stay(x):
        return pltpu.with_memory_space_constraint(x, pltpu.HBM)

    scratch = (
        [
            pltpu.VMEM((S, 2, T, T), F32),
            pltpu.VMEM((2, N, N), F32),
            pltpu.VMEM((B * N, N), F32),
            pltpu.VMEM((2, 4, 2 * N, 2 * N), BF16),
        ]
        + [pltpu.VMEM((2, 3, T + N, N), F32)] * S
        + [
            pltpu.VMEM((S, 2, T, N), F32),
            pltpu.VMEM((S, 2, T, N), F32),
            pltpu.VMEM((S, 2, B * N, N), F32),
            pltpu.VMEM((S - 1, 2, B * N, N), F32),
            pltpu.VMEM((2 * B, 3, 2 * T + N, N), F32),
            pltpu.VMEM((S, 2, 3, T + N, N), F32),
            pltpu.VMEM((S, 2, 2, 3, M, N), F32),
            pltpu.VMEM((S, 2, T, N), F32),
            pltpu.VMEM((S, 2, T, N), F32),
            pltpu.VMEM((2 * N, N), F32),
            pltpu.VMEM((G1, 2 * N // G1, N), F32),
            pltpu.VMEM((YY, 8, N), F32),
            pltpu.VMEM((2 * ZH, 8, N), F32),
            pltpu.VMEM((2 * N // G1, N), F32),
            pltpu.VMEM((8, N), F32),
            pltpu.VMEM((8, N), F32),
            pltpu.VMEM((2 * N // G1, N), F32),
            pltpu.VMEM((2 * N, N), F32),
            pltpu.VMEM((2 * S, 2, M, N), F32),
            pltpu.SMEM((2, B), jnp.int32),
            pltpu.SMEM((B,), jnp.int32),
        ]
        + [dma((S,)), dma((5,)), dma((S,)), dma((9,))]
        + [dma((S, 2)), dma((S,)), dma((S,)), dma((S, 2)), dma((5,)), dma((2 * S,)), dma]
    )
    return pl.pallas_call(
        functools.partial(kernel, n_row, n_col),
        out_shape=(
            jax.ShapeDtypeStruct((S, 2, T, T), F32),
            jax.ShapeDtypeStruct((2, N, N), F32),
        ),
        in_specs=[hbm, hbm, hbm, hbm, hbm, hbm],
        out_specs=(pl.BlockSpec(memory_space=pl.ANY), vmem),
        scratch_shapes=scratch,
        compiler_params=pltpu.CompilerParams(
            collective_id=0, has_side_effects=True, vmem_limit_bytes=VMEM_LIMIT
        ),
        name="step",
    )(
        stay(jnp.transpose(offsets.reshape(B, 2))),
        stay(active_flags.reshape(B)),
        stay(object_slices),
        stay(probe_wave),
        stay(intensity.reshape(B * N, N)),
        stay(jnp.asarray(tables())),
    )


def solution(mesh):
    in_specs = (
        P(None, None, "row", "col"),
        P(),
        P("row", "col", None, None),
        P("row", "col", None),
        P("row", "col", None, None, None),
    )
    out_specs = (P(None, None, "row", "col"), P())
    run = functools.partial(body, mesh.shape["row"], mesh.shape["col"])
    return jax.shard_map(run, mesh=mesh, in_specs=in_specs, out_specs=out_specs, check_vma=False)
```
